32 devices in a mesh: groups: 2 (over y), expert: 4 (over z), tensor: 4 (over x, core).
Axes of the slice: x: 2, y: 2, z: 4, core: 2. Of those that a mesh axis runs over, the one named last changes fastest.
Arguments:
- tokens: bfloat16 [1024, 7168], P(('groups', 'expert'), 'tensor'), parts along dimension 0, may hold values from -6 to 6
- choices: int32 [1024, 4], P(('groups', 'expert')), parts along dimension 0, may hold values from 0 to 15, all different within a row; in each aligned block of 128 rows (0 to 127, 128 to 255, ...) at most 48 rows name the same one
- affinity: float32 [1024, 4], P(('groups', 'expert')), parts along dimension 0, may hold values from -6 to 6
- expert_gate: bfloat16 [7168, 16384], P('tensor', 'expert'), may hold values from -0.0625 to 0.0625
- expert_up: bfloat16 [7168, 16384], P('tensor', 'expert'), may hold values from -0.0625 to 0.0625
- expert_down: bfloat16 [16384, 7168], P('expert', 'tensor'), may hold values from -0.1875 to 0.1875
- shared_in: bfloat16 [2, 1024, 7168], P(None, 'expert', 'tensor'), may hold values from -0.0625 to 0.0625
- shared_down: bfloat16 [1024, 7168], P('expert', 'tensor'), may hold values from -0.1875 to 0.1875
Outputs:
- mixed: bfloat16 [1024, 7168], P(('groups', 'expert'), 'tensor'), parts along dimension 0
The draws below stay inside these ranges and needn't reach their ends.
There are 2 independent parts, one for each index of `groups`. The reference program is written for one: setup_inputs(seed, part) draws one part's arguments, and reference() takes and returns one part's arrays. A program takes and returns all parts, laid end to end along the dimension named above; an argument that names none is the same for every part. Nothing has to cross between parts.
Inputs may be any that keep to these rules, and one draw needn't show every extreme that they name: `choices`: within the rows of one index of expert (128 tokens) every expert is named at most 48 times, a bound that some block reaches; a token names 4 different experts.
All inputs are finite; a program needn't handle non-finite values.
Results may differ from the reference program's by a relative error of at most 0.02.
Values may be sent and summed in bfloat16 or wider, within the bound.
A program may use at most 128 MiB of HBM per device.

```python
import math
import jax
import jax.numpy as jnp
import numpy as np
from jax import lax

D = 7168
FFE = 1024
FS = 1024
EXPERTS = 16
TOP = 4
TOK_DEV = 128
CAP = 48
TOKENS = 512
PIECE = 1024
N_TENSOR = 4


def shard_levels(stream_key, shape, cuts, low, high):
    def one(dim, shards_of):
        draws = jax.random.uniform(jax.random.fold_in(jax.random.fold_in(stream_key, 6), dim), (shards_of,), jnp.float32, low / len(cuts), high / len(cuts))
        return jnp.repeat(jnp.exp(draws), shape[dim] // shards_of).reshape((-1,) + (1,) * (len(shape) - dim - 1))

    factor_of = one(*cuts[0])
    for cut in cuts[1:]:
        factor_of = factor_of * one(*cut)
    return factor_of


def routed_block(own_key, own, number, rows, count, top, limit, skew):
    sequence = jax.random.permutation(own_key, count)
    packed, usual = shares(count, rows * top, limit, skew, True), shares(count, rows * top, limit, skew, False)
    places = jnp.arange(count)

    def named(sizes, rotation):
        used = int((sizes > 0).sum())
        fixed = max(1, used // 4)
        passed = fixed + (places - fixed + rotation * (used - fixed)) % max(1, count - fixed)
        return jnp.zeros((count,), jnp.int32).at[sequence[jnp.where(places < fixed, places, passed)]].set(jnp.asarray(sizes, jnp.int32))

    sizes = jnp.where(number % 4 == 0, named(packed, number // 4), named(usual, number - number // 4 - 1))
    mixed = jax.random.permutation(jax.random.fold_in(own, 3), count)
    donor, taker = mixed[0:count // 2 * 2:2], mixed[1:count // 2 * 2:2]
    margin = jnp.minimum(sizes[donor] - 1, limit - sizes[taker]) // 2
    margin = jnp.where((donor == sequence[0]) | (taker == sequence[0]) | (sizes[taker] == 0), 0, jnp.maximum(margin, 0))
    passed = jax.random.randint(jax.random.fold_in(own, 4), (count // 2,), 0, 1 << 20) % (margin + 1)
    sizes = sizes.at[donor].add(-passed).at[taker].add(passed)
    members = jnp.searchsorted(jnp.cumsum(sizes), jnp.arange(rows * top), side="right").astype(jnp.int32)
    listing = members.reshape(top, rows).T
    listing = listing[jax.random.permutation(jax.random.fold_in(own, 1), rows)]
    rotation = jax.random.randint(jax.random.fold_in(own, 2), (rows, 1), 0, top)
    return jnp.take_along_axis(listing, (jnp.arange(top)[None, :] + rotation) % top, axis=1)


def shares(number_of, total, reach, skew, full):
    loads = [(1 << 20) // math.isqrt(grade ** skew) + 1 for grade in range(1, number_of + 1)]
    largest = reach if full else min(reach, max(-(-total // number_of), total * loads[0] // sum(loads)))
    least = 1 if total - largest >= number_of - 1 else 0
    given, spare = [largest] + [least] * (number_of - 1), total - largest - least * (number_of - 1)
    while spare > 0:
        movable = [i for i in range(1, number_of) if given[i] < largest] or [i for i in range(1, number_of) if given[i] < reach]
        pool, remaining = sum([loads[i] for i in movable]), spare
        for i in movable:
            more = min(reach - given[i], max(1, remaining * loads[i] // pool), spare)
            given[i] = given[i] + more
            spare = spare - more
    return np.array(given)


def noise(own_key, extent, scale, limit, split=(), kind=jnp.bfloat16):
    entries = scale * jax.random.normal(own_key, extent, jnp.float32)
    if split:
        entries = entries * shard_levels(own_key, extent, split, -0.22, 0.18)
    return jnp.clip(entries, -limit, limit).astype(kind)


def setup_inputs(seed: int = 0, part: int = 0) -> dict:
    seeds = jax.random.split(jax.random.key(seed), 9)
    part_keys = jax.random.split(jax.random.fold_in(seeds[8], part), 9)
    tokens = noise(part_keys[0], (TOKENS, D), 1.0, 6.0, ((0, 4), (1, 4)))
    choices_keys = jax.random.split(jax.random.fold_in(part_keys[1], 1), TOKENS // TOK_DEV)
    choices_turns = jax.random.permutation(jax.random.fold_in(part_keys[1], 3), TOKENS // TOK_DEV)
    choices = jax.vmap(lambda own, number: routed_block(jax.random.fold_in(part_keys[1], 2), own, number, TOK_DEV, EXPERTS, TOP, CAP, 2))(choices_keys, choices_turns).reshape((TOKENS, TOP))
    affinity = noise(part_keys[2], (TOKENS, TOP), 1.5, 6.0, ((0, 4),), jnp.float32)
    expert_gate = noise(seeds[3], (D, EXPERTS * FFE), D ** -0.5, 0.0625, ((0, 4), (1, 4)))
    expert_up = noise(seeds[4], (D, EXPERTS * FFE), D ** -0.5, 0.0625, ((0, 4), (1, 4)))
    expert_down = noise(seeds[5], (EXPERTS * FFE, D), FFE ** -0.5, 0.1875, ((0, 4), (1, 4)))
    shared_in = noise(seeds[6], (2, FS, D), D ** -0.5, 0.0625, ((1, 4), (2, 4)))
    shared_down = noise(seeds[7], (FS, D), FS ** -0.5, 0.1875, ((0, 4), (1, 4)))
    return dict(tokens=tokens, choices=choices, affinity=affinity, expert_gate=expert_gate, expert_up=expert_up, expert_down=expert_down, shared_in=shared_in, shared_down=shared_down)


def tensor_partials(feature_slices, weight):
    width = weight.shape[1]
    slices = weight.astype(jnp.float32).reshape(N_TENSOR, D // N_TENSOR, width)
    parts = jnp.einsum("tnd,ndk->ntk", feature_slices, slices, precision=lax.Precision.HIGHEST)
    rounded = lax.optimization_barrier(parts.astype(jnp.bfloat16))
    return jnp.sum(rounded.astype(jnp.float32), axis=0)


def reference(tokens, choices, affinity, expert_gate, expert_up, expert_down, shared_in, shared_down):
    split_count = FFE // PIECE
    feature_slices = tokens.astype(jnp.float32).reshape(TOKENS, N_TENSOR, D // N_TENSOR)
    sigmoids = jax.nn.sigmoid(affinity)
    mix = 2.5 * sigmoids / jnp.sum(sigmoids, axis=1, keepdims=True)
    gate_all = jnp.transpose(expert_gate.reshape(D, EXPERTS, FFE), (1, 0, 2))
    up_all = jnp.transpose(expert_up.reshape(D, EXPERTS, FFE), (1, 0, 2))
    down_all = expert_down.reshape(EXPERTS, split_count, PIECE, D)

    def one_expert(running, inputs):
        gate_cols, up_cols, down_rows, index = inputs
        gate = tensor_partials(feature_slices, gate_cols)
        upper = tensor_partials(feature_slices, up_cols)
        hidden = (jax.nn.silu(gate) * upper).astype(jnp.bfloat16)
        hidden_pieces = hidden.astype(jnp.float32).reshape(TOKENS, split_count, PIECE)
        pieces = jnp.einsum("tsp,spd->tsd", hidden_pieces, down_rows.astype(jnp.float32), precision=lax.Precision.HIGHEST)
        rounded = lax.optimization_barrier(pieces.astype(jnp.bfloat16))
        expert_out = jnp.sum(rounded.astype(jnp.float32), axis=1)
        share = jnp.sum(jnp.where(choices == index, mix, 0.0), axis=1)
        return running + share[:, None] * expert_out, None

    indices = jnp.arange(EXPERTS).astype(jnp.int32)
    start = jnp.zeros((TOKENS, D), jnp.float32)
    routed, unused = lax.scan(one_expert, start, (gate_all, up_all, down_all, indices))
    shared_gate = tensor_partials(feature_slices, jnp.transpose(shared_in[0]))
    shared_up = tensor_partials(feature_slices, jnp.transpose(shared_in[1]))
    shared_hidden = (jax.nn.silu(shared_gate) * shared_up).astype(jnp.bfloat16)
    shared_out = jnp.dot(shared_hidden, shared_down, preferred_element_type=jnp.float32)
    return (routed + shared_out).astype(jnp.bfloat16)
```

```python
import functools

import jax
import jax.numpy as jnp
from jax import lax
from jax.experimental import pallas as pl
from jax.experimental.pallas import tpu as pltpu
from jax.sharding import PartitionSpec as P

FFE = 1024
CAP = 48
MESH = pl.DeviceIdType.MESH
F32 = jnp.float32
BF16 = jnp.bfloat16


def mm(a, b, ca=1, cb=0):
    return lax.dot_general(a, b, (((ca,), (cb,)), ((), ())), preferred_element_type=F32)


def ring_rows(tok, hops, hop, rightward):
    if hop < hops:
        return 0, tok
    return (0, tok // 2) if rightward else (tok // 2, tok // 2)


def layer(
    dims, tokens, meta, gate_hbm, up_hbm, down_hbm, sin_hbm, sdown_hbm, out,
    x_all, meta_all, gate_w, up_w, down_w, sin_w, sdown_w, rows_buf, comb,
    part, core_in, x_out, x_in, hid, s_part, s_core_in, s_x_out, s_x_in, s_hid,
    rs_out, rs_in,
    load_sem, gate_sem, up_sem, down_sem, meta_sem, ag_sem, core_sem, x_sem, hx_sem, hc_sem, rs_sem,
):
    ns, nx, local_count, piece, tok, cap, top = dims
    hops = ns // 2
    z, t = lax.axis_index("expert"), lax.axis_index("tensor")
    x, c = lax.div(t, 2), lax.rem(t, 2)
    peer_c = 1 - c
    peer_t = 2 * x + peer_c
    right, left = lax.rem(z + 1, ns), lax.rem(z + ns - 1, ns)
    slots = gate_w.shape[0]

    def zoff(k):
        return lax.rem(z + k + ns, ns)

    def remote(src, dst, sems, index, where):
        send = sems.at[(0,) + index]
        recv = sems.at[(1,) + index]
        return pltpu.make_async_remote_copy(
            src_ref=src, dst_ref=dst, send_sem=send, recv_sem=recv, device_id=where, device_id_type=MESH
        )

    own_tok = pltpu.make_async_copy(tokens, x_all.at[z], load_sem.at[0])
    own_meta = pltpu.make_async_copy(meta, meta_all.at[z], load_sem.at[1])
    own_tok.start()
    own_meta.start()
    barrier = pltpu.get_barrier_semaphore()
    for k in range(1, ns):
        pl.semaphore_signal(barrier, inc=1, device_id={"expert": zoff(k)}, device_id_type=MESH)
    for k in range(1, nx):
        pl.semaphore_signal(
            barrier, inc=1, device_id={"tensor": 2 * lax.rem(x + k, nx) + c}, device_id_type=MESH
        )
    pl.semaphore_signal(barrier, inc=1, device_id={"tensor": peer_t}, device_id_type=MESH)

    sin_load = pltpu.make_async_copy(sin_hbm, sin_w, load_sem.at[2])
    sdown_load = pltpu.make_async_copy(sdown_hbm, sdown_w, load_sem.at[3])
    sin_load.start()

    def cols(e):
        return pl.ds(e * piece, piece)

    gate_loads = [
        pltpu.make_async_copy(gate_hbm.at[:, cols(e)], gate_w.at[e % slots], gate_sem.at[e])
        for e in range(local_count)
    ]
    up_loads = [
        pltpu.make_async_copy(up_hbm.at[:, cols(e)], up_w.at[e % slots], up_sem.at[e])
        for e in range(local_count)
    ]
    down_loads = [
        pltpu.make_async_copy(down_hbm.at[cols(e), :], down_w.at[e], down_sem.at[e])
        for e in range(local_count)
    ]
    own_tok.wait()
    own_meta.wait()
    pl.semaphore_wait(barrier, (ns - 1) + (nx - 1) + 1)

    def ag_copy(hop, rightward):
        start, size = ring_rows(tok, hops, hop, rightward)
        block = zoff(1 - hop) if rightward else zoff(hop - 1)
        ref = x_all.at[block, pl.ds(start, size), :]
        where = {"expert": right if rightward else left}
        return remote(ref, ref, ag_sem, (0 if rightward else 1, hop - 1), where)

    ag = {(h, d): ag_copy(h, d) for h in range(1, hops + 1) for d in (True, False)}
    for d in (True, False):
        ag[1, d].start()
    meta_copies = []
    for k in range(1, ns):
        copy = remote(meta_all.at[z], meta_all.at[z], meta_sem, (k - 1,), {"expert": zoff(k)})
        copy.start()
        meta_copies.append(copy)
    for e in range(min(slots, local_count)):
        gate_loads[e].start()
        up_loads[e].start()
    for e in range(local_count):
        down_loads[e].start()
    sdown_load.start()

    tri = (
        lax.broadcasted_iota(jnp.int32, (tok, tok), 0) < lax.broadcasted_iota(jnp.int32, (tok, tok), 1)
    ).astype(F32).astype(BF16)
    slot_of = lax.broadcasted_iota(jnp.int32, (cap, tok), 0).astype(F32)
    mask_rows = -(-local_count // 8) * 8
    row_of = lax.broadcasted_iota(jnp.int32, (mask_rows, tok), 0)
    columns = local_count * piece

    def dispatch(s):
        info = meta_all[s]
        masks, weights = [], []
        mask_all = jnp.zeros((mask_rows, tok), F32)
        for l in range(local_count):
            eid = lax.div(z * columns + l * piece, FFE).astype(F32)
            hit = (info[:top] == eid).astype(F32)
            mask = jnp.sum(hit, axis=0, keepdims=True)
            masks.append(mask)
            weights.append(jnp.sum(hit * info[top : 2 * top], axis=0, keepdims=True))
            mask_all = jnp.where(row_of == l, mask, mask_all)
        position = mm(mask_all.astype(BF16), tri)
        picks = []
        for l in range(local_count):
            pick = jnp.where((slot_of == position[l : l + 1]) & (masks[l] > 0.5), 1.0, 0.0)
            picks.append(pick.astype(BF16))
            comb[s, pl.ds(l * cap, cap), :] = (pick * weights[l]).astype(BF16)
        stacked = jnp.concatenate(picks, axis=0) if local_count > 1 else picks[0]
        gathered = mm(stacked, x_all[s]).astype(BF16)
        for l in range(local_count):
            rows_buf[l, s] = gathered[l * cap : (l + 1) * cap]

    for copy in meta_copies:
        copy.wait()
    dispatch(z)
    for hop in range(1, hops + 1):
        for d in (True, False):
            ag[hop, d].wait()
            if hop < hops:
                ag[hop + 1, d].start()
        dispatch(zoff(-hop))
        if hop < hops:
            dispatch(zoff(hop))

    unit_count = local_count + 1

    def unit(u):
        if u == 0:
            return s_part, s_core_in, s_x_out, s_x_in, s_hid
        e = u - 1
        return part.at[e], core_in.at[e], x_out.at[e], x_in.at[e], hid.at[e]

    def first(u):
        p, ci, _, _, _ = unit(u)
        if u == 0:
            sin_load.wait()
            whole = x_all[...].reshape(ns * tok, x_all.shape[2])
            for g in range(2):
                p[g] = mm(whole, sin_w[g], 1, 1).astype(BF16)
        else:
            e = u - 1
            lhs = rows_buf[e].reshape(ns * cap, x_all.shape[2])
            gate_loads[e].wait()
            p[0] = mm(lhs, gate_w[e % slots]).astype(BF16)
            up_loads[e].wait()
            p[1] = mm(lhs, up_w[e % slots]).astype(BF16)
            if e + slots < local_count:
                gate_loads[e + slots].start()
                up_loads[e + slots].start()
        half = p.shape[1] // 2
        theirs = pl.ds(pl.multiple_of(peer_c * half, half), half)
        copy = remote(p.at[:, theirs, :], ci, core_sem, (u,), {"tensor": peer_t})
        copy.start()
        return copy

    def chunk(p, ci, which):
        half = p.shape[1] // 2
        q = half // nx
        mine = pl.ds(pl.multiple_of(c * half + which * q, q), q)
        there = pl.ds(pl.multiple_of(which * q, q), q)
        return [p[g, mine, :].astype(F32) + ci[g, there, :].astype(F32) for g in range(2)]

    def second(u, core_copy):
        p, ci, xo, xi, _ = unit(u)
        core_copy.wait()
        copies = []
        for k in range(1, nx):
            other = lax.rem(x + k, nx)
            sums = chunk(p, ci, other)
            for g in range(2):
                xo[k - 1, g] = sums[g].astype(BF16)
            copy = remote(xo.at[k - 1], xi.at[k - 1], x_sem, (u, k - 1), {"tensor": 2 * other + c})
            copy.start()
            copies.append(copy)
        return copies

    def hid_rows(h, which):
        half = h.shape[0] // 2
        q = half // nx
        return h.at[pl.ds(pl.multiple_of(c * half + which * q, q), q), :]

    def third(u, x_copies):
        p, ci, _, xi, h = unit(u)
        sums = chunk(p, ci, x)
        for k in range(1, nx):
            x_copies[k - 1].wait()
            for g in range(2):
                sums[g] = sums[g] + xi[k - 1, g].astype(F32)
        gate, up = sums
        value = (gate / (1.0 + jnp.exp(-gate)) * up).astype(BF16)
        ref = hid_rows(h, x)
        ref[...] = value
        x_sends = []
        for k in range(1, nx):
            where = {"tensor": 2 * lax.rem(x + k, nx) + c}
            copy = remote(ref, ref, hx_sem, (u, k - 1), where)
            copy.start()
            x_sends.append(copy)
        copy = remote(ref, ref, hc_sem, (u, 0), {"tensor": peer_t})
        copy.start()
        return x_sends, [copy]

    def fourth(u, x_sends, core_sends):
        h = unit(u)[4]
        for k in range(1, nx):
            x_sends[k - 1].wait()
            ref = hid_rows(h, lax.rem(x + nx - k, nx))
            copy = remote(ref, ref, hc_sem, (u, k), {"tensor": peer_t})
            copy.start()
            core_sends.append(copy)
        return core_sends

    def fifth(u, core_sends):
        for copy in core_sends:
            copy.wait()
        if u > 0:
            e = u - 1
            down_loads[e].wait()
            made = mm(hid[e], down_w[e]).astype(BF16)
            rows_buf[e] = made.reshape(ns, cap, made.shape[1])

    state = {}
    for u in range(unit_count + 1):
        if u < unit_count:
            state[u] = first(u)
        if u >= 1:
            state[u - 1] = second(u - 1, state[u - 1])
    for u in range(unit_count + 2):
        if u < unit_count:
            state[u] = third(u, state[u])
        if 1 <= u <= unit_count:
            state[u - 1] = fourth(u - 1, *state[u - 1])
        if u >= 2:
            fifth(u - 2, state[u - 2])

    sdown_load.wait()

    def partial(s):
        made = rows_buf[:, s].reshape(local_count * cap, x_all.shape[2])
        shared = s_hid[pl.ds(pl.multiple_of(s * tok, tok), tok), :]
        return mm(comb[s], made, 0, 0) + mm(shared, sdown_w[...])

    def rs_copy(hop, rightward):
        start, size = ring_rows(tok, hops, hop, rightward)
        d = 0 if rightward else 1
        span = pl.ds(start, size)
        where = {"expert": right if rightward else left}
        return remote(
            rs_out.at[d, hop - 1, span, :], rs_in.at[d, hop - 1, span, :], rs_sem, (d, hop - 1), where
        )

    def arrived(hop, rightward):
        start, size = ring_rows(tok, hops, hop, rightward)
        got = rs_in[0 if rightward else 1, hop - 1, pl.ds(start, size), :].astype(F32)
        if size == tok:
            return got
        fill = jnp.zeros((tok - size, got.shape[1]), F32)
        return jnp.concatenate([got, fill] if start == 0 else [fill, got], axis=0)

    rs = {(h, d): rs_copy(h, d) for h in range(1, hops + 1) for d in (True, False)}
    opposite = partial(zoff(hops)).astype(BF16)
    for d in (True, False):
        start, size = ring_rows(tok, hops, hops, d)
        rs_out[0 if d else 1, hops - 1, pl.ds(start, size), :] = opposite[start : start + size]
        rs[hops, d].start()
    for hop in range(hops - 1, 0, -1):
        for d in (True, False):
            value = partial(zoff(hop if d else -hop))
            rs[hop + 1, d].wait()
            rs_out[0 if d else 1, hop - 1] = (value + arrived(hop + 1, d)).astype(BF16)
            rs[hop, d].start()
    total = partial(z)
    for d in (True, False):
        rs[1, d].wait()
        total = total + arrived(1, d)
    out[...] = total.astype(BF16)


def line_layer(
    dims, tokens, meta, gate_hbm, up_hbm, down_hbm, sin_hbm, sdown_hbm, out,
    x_all, meta_all, gate_w, up_w, down_w, sin_w, sdown_w, rows, made, comb,
    part, core_in, x_out, x_in, hid, s_part, s_core_in, s_x_out, s_x_in, s_hid, rs_in,
    load_sem, gate_sem, up_sem, down_sem, meta_sem, ag_sem, core_sem, x_sem, hx_sem, hc_sem, rs_sem,
):
    ns, nx, local_count, piece, tok, cap, top, pieces, cw = dims
    width = x_all.shape[2]
    z, t = lax.axis_index("expert"), lax.axis_index("tensor")
    x, c = lax.div(t, 2), lax.rem(t, 2)
    peer_c = 1 - c
    peer_t = 2 * x + peer_c
    mir = lax.div(z, ns // 2)
    zeta = z + mir * (ns - 1 - 2 * z)
    above = z + 1 - 2 * mir
    below = z - 1 + 2 * mir
    spread = tok // pieces

    def phys(b):
        return b + mir * (ns - 1 - 2 * b)

    def zoff(k):
        return lax.rem(z + k + ns, ns)

    def remote(src, dst, sems, index, where):
        send = sems.at[(0,) + index]
        recv = sems.at[(1,) + index]
        return pltpu.make_async_remote_copy(
            src_ref=src, dst_ref=dst, send_sem=send, recv_sem=recv, device_id=where, device_id_type=MESH
        )

    own_tok = pltpu.make_async_copy(tokens, x_all.at[z], load_sem.at[0])
    own_meta = pltpu.make_async_copy(meta, meta_all.at[z], load_sem.at[1])
    own_tok.start()
    own_meta.start()
    barrier = pltpu.get_barrier_semaphore()
    for k in range(1, ns):
        pl.semaphore_signal(barrier, inc=1, device_id={"expert": zoff(k)}, device_id_type=MESH)
    for k in range(1, nx):
        pl.semaphore_signal(
            barrier, inc=1, device_id={"tensor": 2 * lax.rem(x + k, nx) + c}, device_id_type=MESH
        )
    pl.semaphore_signal(barrier, inc=1, device_id={"tensor": peer_t}, device_id_type=MESH)

    sin_load = pltpu.make_async_copy(sin_hbm, sin_w, load_sem.at[2])
    sdown_load = pltpu.make_async_copy(sdown_hbm, sdown_w, load_sem.at[3])

    def cols(e):
        return pl.ds(e * piece, piece)

    gate_loads = [
        pltpu.make_async_copy(gate_hbm.at[:, cols(e)], gate_w.at[e], gate_sem.at[e]) for e in range(local_count)
    ]
    up_loads = [
        pltpu.make_async_copy(up_hbm.at[:, cols(e)], up_w.at[e], up_sem.at[e]) for e in range(local_count)
    ]
    down_loads = [
        pltpu.make_async_copy(down_hbm.at[cols(e), :], down_w.at[e], down_sem.at[e]) for e in range(local_count)
    ]
    sin_load.start()
    for e in range(local_count):
        gate_loads[e].start()
        up_loads[e].start()
    for e in range(local_count):
        down_loads[e].start()
    sdown_load.start()
    own_tok.wait()
    own_meta.wait()
    pl.semaphore_wait(barrier, (ns - 1) + (nx - 1) + 1)

    def ag_copy(upward, b, k, where):
        d = mir if upward else 1 - mir
        block = phys(b)
        ref = x_all.at[block, pl.ds(k * spread, spread), :]
        return remote(ref, ref, ag_sem, (d, block, k), {"expert": where})

    for k in range(pieces):
        ag_copy(True, zeta, k, above).start()

        @pl.when(zeta > 0)
        def _():
            ag_copy(False, zeta, k, below).start()

    meta_copies = []
    for k in range(1, ns):
        copy = remote(meta_all.at[z], meta_all.at[z], meta_sem, (k - 1,), {"expert": zoff(k)})
        copy.start()
        meta_copies.append(copy)

    def from_above(b, k):
        ag_copy(False, b, k, above).wait_recv()

        @pl.when(zeta > 0)
        def _():
            ag_copy(False, b, k, below).start()

    def from_below(b, k):
        ag_copy(True, b, k, above).wait_recv()
        ag_copy(True, b, k, above).start()

    def arrive(i, k):
        far = (i + 1) // 2
        if i % 2:
            @pl.when(2 * zeta >= i)
            def _():
                from_below(zeta - far, k)
                from_above(zeta + far, k)

        @pl.when(2 * zeta < i)
        def _():
            from_above(i, k)

    def step_block(i):
        if i == 0:
            return z
        near = lax.div(2 * zeta - i + ns, ns)
        side = zeta - (i + 1) // 2 if i % 2 else zeta + i // 2
        return phys(near * side + (1 - near) * i)

    tri = (
        lax.broadcasted_iota(jnp.int32, (tok, tok), 0) < lax.broadcasted_iota(jnp.int32, (tok, tok), 1)
    ).astype(F32).astype(BF16)
    slot_of = lax.broadcasted_iota(jnp.int32, (cap, tok), 0).astype(F32)
    mask_rows = -(-local_count // 8) * 8
    row_of = lax.broadcasted_iota(jnp.int32, (mask_rows, tok), 0)
    columns = local_count * piece

    def dispatch(s):
        info = meta_all[s]
        masks, weights = [], []
        mask_all = jnp.zeros((mask_rows, tok), F32)
        for l in range(local_count):
            eid = lax.div(z * columns + l * piece, FFE).astype(F32)
            hit = (info[:top] == eid).astype(F32)
            mask = jnp.sum(hit, axis=0, keepdims=True)
            masks.append(mask)
            weights.append(jnp.sum(hit * info[top : 2 * top], axis=0, keepdims=True))
            mask_all = jnp.where(row_of == l, mask, mask_all)
        position = mm(mask_all.astype(BF16), tri)
        picks = []
        for l in range(local_count):
            pick = jnp.where((slot_of == position[l : l + 1]) & (masks[l] > 0.5), 1.0, 0.0)
            picks.append(pick.astype(BF16))
            comb[s, pl.ds(l * cap, cap), :] = (pick * weights[l]).astype(BF16)
        stacked = jnp.concatenate(picks, axis=0) if local_count > 1 else picks[0]
        gathered = mm(stacked, x_all[s]).astype(BF16)
        for l in range(local_count):
            rows[l] = gathered[l * cap : (l + 1) * cap]

    units = local_count + 1

    def refs(i, u):
        if u == 0:
            return (
                s_part.at[i % 2], s_core_in.at[i], s_x_out.at[i], s_x_in.at[i], s_hid.at[step_block(i)]
            )
        e = u - 1
        return part.at[i % 2, e], core_in.at[i, e], x_out.at[i, e], x_in.at[i, e], hid.at[i, e]

    def along(u, start, size, lead):
        step = pl.ds(pl.multiple_of(start, size), size)
        return lead + ((step, slice(None)) if u == 0 else (slice(None), step))

    def extent(u):
        return tok if u == 0 else piece

    def first(i, u):
        p, ci = refs(i, u)[:2]
        if u == 0:
            if i == 0:
                sin_load.wait()
            block = x_all[step_block(i)]
            for g in range(2):
                p[g] = mm(block, sin_w[g], 1, 1).astype(BF16)
        else:
            e = u - 1
            lhs = rows[e]
            if i == 0:
                gate_loads[e].wait()
            p[0] = mm(lhs, gate_w[e]).astype(BF16)
            if i == 0:
                up_loads[e].wait()
            p[1] = mm(lhs, up_w[e]).astype(BF16)
        half = extent(u) // 2
        theirs = along(u, peer_c * half, half, (slice(None),))
        copy = remote(p.at[theirs], ci, core_sem, (i, u), {"tensor": peer_t})
        copy.start()
        return copy

    def chunk(i, u, which):
        p, ci = refs(i, u)[:2]
        half = extent(u) // 2
        q = half // nx
        sums = []
        for g in range(2):
            mine = p[along(u, c * half + which * q, q, (g,))].astype(F32)
            sums.append(mine + ci[along(u, which * q, q, (g,))].astype(F32))
        return sums

    def second(i, u, core_copy):
        _, _, xo, xi, _ = refs(i, u)
        core_copy.wait()
        copies = []
        for k in range(1, nx):
            other = lax.rem(x + k, nx)
            sums = chunk(i, u, other)
            for g in range(2):
                xo[k - 1, g] = sums[g].astype(BF16)
            copy = remote(xo.at[k - 1], xi.at[k - 1], x_sem, (i, u, k - 1), {"tensor": 2 * other + c})
            copy.start()
            copies.append(copy)
        return copies

    def hid_part(i, u, which):
        half = extent(u) // 2
        q = half // nx
        return refs(i, u)[4].at[along(u, c * half + which * q, q, ())]

    def third(i, u, x_copies):
        xi = refs(i, u)[3]
        sums = chunk(i, u, x)
        for k in range(1, nx):
            x_copies[k - 1].wait()
            for g in range(2):
                sums[g] = sums[g] + xi[k - 1, g].astype(F32)
        gate, up = sums
        value = (gate / (1.0 + jnp.exp(-gate)) * up).astype(BF16)
        ref = hid_part(i, u, x)
        ref[...] = value
        x_sends = []
        for k in range(1, nx):
            where = {"tensor": 2 * lax.rem(x + k, nx) + c}
            copy = remote(ref, ref, hx_sem, (i, u, k - 1), where)
            copy.start()
            x_sends.append(copy)
        copy = remote(ref, ref, hc_sem, (i, u, 0), {"tensor": peer_t})
        copy.start()
        return x_sends, [copy]

    def fourth(i, u, x_sends, core_sends):
        for k in range(1, nx):
            x_sends[k - 1].wait()
            ref = hid_part(i, u, lax.rem(x + nx - k, nx))
            copy = remote(ref, ref, hc_sem, (i, u, k), {"tensor": peer_t})
            copy.start()
            core_sends.append(copy)
        return core_sends

    def fifth(i, u, core_sends):
        for copy in core_sends:
            copy.wait()
        if u > 0:
            e = u - 1
            if i == 0:
                down_loads[e].wait()
            made[step_block(i), pl.ds(e * cap, cap), :] = mm(hid[i, e], down_w[e]).astype(BF16)
        elif i == 0:
            sdown_load.wait()

    parts = width // cw

    def contribution(b, k):
        span = pl.ds(k * cw, cw)
        return mm(comb[b], made[b, :, span], 0, 0) + mm(s_hid[b], sdown_w[:, span])

    def rs_copy(upward, b, k, where):
        d = mir if upward else 1 - mir
        block = phys(b)
        slot = block + 1 - d
        span = pl.ds(k * cw, cw)
        return remote(
            x_all.at[block, :, span], rs_in.at[slot, :, span], rs_sem, (slot, k), {"expert": where}
        )

    def arrived(upward, b, k):
        rs_copy(upward, b, k, above).wait_recv()
        d = mir if upward else 1 - mir
        return rs_in[phys(b) + 1 - d, :, pl.ds(k * cw, cw)].astype(F32)

    def originate(r):
        @pl.when(zeta == 0)
        def _():
            for k in range(parts):
                x_all[phys(r), :, pl.ds(k * cw, cw)] = contribution(phys(r), k).astype(BF16)
                rs_copy(True, r, k, above).start()

    def relay(upward, b, k):
        value = contribution(phys(b), k)
        total = value + arrived(upward, b, k)
        x_all[phys(b), :, pl.ds(k * cw, cw)] = total.astype(BF16)
        rs_copy(upward, b, k, above if upward else below).start()

    state = {}

    def run(name, i, u):
        if name == "A":
            state[i, u] = first(i, u)
        elif name == "B":
            state[i, u] = second(i, u, state[i, u])
        elif name == "C":
            state[i, u] = third(i, u, state[i, u])
        elif name == "D":
            state[i, u] = fourth(i, u, *state[i, u])
        else:
            fifth(i, u, state[i, u])

    mid = units // 2
    for i in range(ns):
        if i > 0:
            for k in range(pieces):
                if k == 0:
                    pl.when(zeta == 0)(functools.partial(arrive, i, k))
                else:
                    arrive(i, k)
            if i == 1:
                for copy in meta_copies:
                    copy.wait()
        dispatch(step_block(i))
        behind = []
        if i > 0:
            behind = [("D", u) for u in range(units)] + [("E", u) for u in range(units)]
        per = -(-len(behind) // max(1, units - 1))
        for u in range(units):
            run("A", i, u)
            if u > 0:
                run("B", i, u - 1)
                for name, v in behind[(u - 1) * per : u * per]:
                    run(name, i - 1, v)
            if u >= 3:
                run("C", i, u - 3)
            if u == mid and i + 1 < ns:
                pl.when(zeta > 0)(functools.partial(arrive, i + 1, 0))
        if i > 1:
            originate(i - 1)
        run("B", i, units - 1)
        tail = list(range(max(0, units - 3), units))
        if i + 1 < ns:
            for u in tail:
                run("C", i, u)
        else:
            for u in tail:
                run("C", i, u)
                run("D", i, u - tail[0])
            for u in range(units):
                if u + len(tail) < units:
                    run("D", i, u + len(tail))
                run("E", i, u)
    originate(ns - 1)

    @pl.when(zeta > 0)
    def _():
        for k in range(pieces):
            ag_copy(True, zeta, k, above).wait_send()
            ag_copy(False, zeta, k, below).wait_send()
            for b in range(ns):
                @pl.when(b < zeta)
                def _():
                    ag_copy(True, b, k, above).wait_send()

                @pl.when(b > zeta)
                def _():
                    ag_copy(False, b, k, below).wait_send()

    for r in range(1, ns):
        for k in range(parts + 2):
            if k < parts:
                pl.when((zeta > 0) & (zeta < r))(functools.partial(relay, True, r, k))
            if k >= 2:
                pl.when(zeta > ns - 1 - r)(functools.partial(relay, False, ns - 1 - r, k - 2))

    for k in range(parts):
        span = pl.ds(k * cw, cw)
        value = contribution(z, k) + arrived(False, zeta, k)

        @pl.when(zeta == 0)
        def _():
            out[:, span] = value.astype(BF16)

        @pl.when(zeta > 0)
        def _():
            out[:, span] = (value + arrived(True, zeta, k)).astype(BF16)

    @pl.when(zeta == 0)
    def _():
        for k in range(pieces):
            ag_copy(True, zeta, k, above).wait_send()

    for b in range(ns):
        for k in range(parts):
            @pl.when(zeta < b)
            def _():
                rs_copy(True, b, k, above).wait_send()

            @pl.when(zeta > b)
            def _():
                rs_copy(False, b, k, above).wait_send()


def local(tokens, choices, affinity, expert_gate, expert_up, expert_down, shared_in, shared_down):
    tok, width = tokens.shape
    top = choices.shape[1]
    ns, nt = lax.axis_size("expert"), lax.axis_size("tensor")
    nx = nt // 2
    piece = min(FFE, expert_gate.shape[1])
    local_count = expert_gate.shape[1] // piece
    hs = shared_in.shape[1]
    hops = ns // 2
    slots = min(3, local_count)
    sigmoids = jax.nn.sigmoid(affinity)
    mix = 2.5 * sigmoids / jnp.sum(sigmoids, axis=1, keepdims=True)
    meta = jnp.concatenate([choices.astype(F32).T, mix.T], axis=0)
    rows = ns * CAP
    srows = ns * tok
    units = local_count + 1
    dims = (ns, nx, local_count, piece, tok, CAP, top)
    hbm = pl.BlockSpec(memory_space=pl.ANY)
    sem = pltpu.SemaphoreType.DMA
    scratch = [
        pltpu.VMEM((ns, tok, width), BF16),
        pltpu.VMEM((ns,) + meta.shape, F32),
        pltpu.VMEM((slots, width, piece), BF16),
        pltpu.VMEM((slots, width, piece), BF16),
        pltpu.VMEM((local_count, piece, width), BF16),
        pltpu.VMEM(shared_in.shape, BF16),
        pltpu.VMEM(shared_down.shape, BF16),
        pltpu.VMEM((local_count, ns, CAP, width), BF16),
        pltpu.VMEM((ns, local_count * CAP, tok), BF16),
        pltpu.VMEM((local_count, 2, rows, piece), BF16),
        pltpu.VMEM((local_count, 2, rows // 2, piece), BF16),
        pltpu.VMEM((local_count, nx - 1, 2, rows // nt, piece), BF16),
        pltpu.VMEM((local_count, nx - 1, 2, rows // nt, piece), BF16),
        pltpu.VMEM((local_count, rows, piece), BF16),
        pltpu.VMEM((2, srows, hs), BF16),
        pltpu.VMEM((2, srows // 2, hs), BF16),
        pltpu.VMEM((nx - 1, 2, srows // nt, hs), BF16),
        pltpu.VMEM((nx - 1, 2, srows // nt, hs), BF16),
        pltpu.VMEM((srows, hs), BF16),
        pltpu.VMEM((2, hops, tok, width), BF16),
        pltpu.VMEM((2, hops, tok, width), BF16),
        sem((4,)),
        sem((local_count,)),
        sem((local_count,)),
        sem((local_count,)),
        sem((2, ns - 1)),
        sem((2, 2, hops)),
        sem((2, units)),
        sem((2, units, nx - 1)),
        sem((2, units, nx - 1)),
        sem((2, units, nx)),
        sem((2, 2, hops)),
    ]
    return pl.pallas_call(
        functools.partial(layer, dims),
        out_shape=jax.ShapeDtypeStruct((tok, width), BF16),
        in_specs=[hbm] * 7,
        out_specs=pl.BlockSpec(memory_space=pltpu.VMEM),
        scratch_shapes=scratch,
        compiler_params=pltpu.CompilerParams(
            collective_id=0, has_side_effects=True, vmem_limit_bytes=60 * 1024 * 1024
        ),
        name="moe_layer",
    )(tokens, meta, expert_gate, expert_up, expert_down, shared_in, shared_down)


def line_local(tokens, choices, affinity, expert_gate, expert_up, expert_down, shared_in, shared_down):
    tok, width = tokens.shape
    top = choices.shape[1]
    ns, nt = lax.axis_size("expert"), lax.axis_size("tensor")
    nx = nt // 2
    piece = min(FFE, expert_gate.shape[1])
    local_count = expert_gate.shape[1] // piece
    hs = shared_in.shape[1]
    pieces = 2
    cw = 256 if width % 256 == 0 else 128
    sigmoids = jax.nn.sigmoid(affinity)
    mix = 2.5 * sigmoids / jnp.sum(sigmoids, axis=1, keepdims=True)
    meta = jnp.concatenate([choices.astype(F32).T, mix.T], axis=0)
    units = local_count + 1
    dims = (ns, nx, local_count, piece, tok, CAP, top, pieces, cw)
    hbm = pl.BlockSpec(memory_space=pl.ANY)
    sem = pltpu.SemaphoreType.DMA
    scratch = [
        pltpu.VMEM((ns, tok, width), BF16),
        pltpu.VMEM((ns,) + meta.shape, F32),
        pltpu.VMEM((local_count, width, piece), BF16),
        pltpu.VMEM((local_count, width, piece), BF16),
        pltpu.VMEM((local_count, piece, width), BF16),
        pltpu.VMEM(shared_in.shape, BF16),
        pltpu.VMEM(shared_down.shape, BF16),
        pltpu.VMEM((local_count, CAP, width), BF16),
        pltpu.VMEM((ns, local_count * CAP, width), BF16),
        pltpu.VMEM((ns, local_count * CAP, tok), BF16),
        pltpu.VMEM((2, local_count, 2, CAP, piece), BF16),
        pltpu.VMEM((ns, local_count, 2, CAP, piece // 2), BF16),
        pltpu.VMEM((ns, local_count, nx - 1, 2, CAP, piece // nt), BF16),
        pltpu.VMEM((ns, local_count, nx - 1, 2, CAP, piece // nt), BF16),
        pltpu.VMEM((ns, local_count, CAP, piece), BF16),
        pltpu.VMEM((2, 2, tok, hs), BF16),
        pltpu.VMEM((ns, 2, tok // 2, hs), BF16),
        pltpu.VMEM((ns, nx - 1, 2, tok // nt, hs), BF16),
        pltpu.VMEM((ns, nx - 1, 2, tok // nt, hs), BF16),
        pltpu.VMEM((ns, tok, hs), BF16),
        pltpu.VMEM((ns + 1, tok, width), BF16),
        sem((4,)),
        sem((local_count,)),
        sem((local_count,)),
        sem((local_count,)),
        sem((2, ns - 1)),
        sem((2, 2, ns, pieces)),
        sem((2, ns, units)),
        sem((2, ns, units, nx - 1)),
        sem((2, ns, units, nx - 1)),
        sem((2, ns, units, nx)),
        sem((2, ns + 1, width // cw)),
    ]
    return pl.pallas_call(
        functools.partial(line_layer, dims),
        out_shape=jax.ShapeDtypeStruct((tok, width), BF16),
        in_specs=[hbm] * 7,
        out_specs=pl.BlockSpec(memory_space=pltpu.VMEM),
        scratch_shapes=scratch,
        compiler_params=pltpu.CompilerParams(
            collective_id=0, has_side_effects=True, vmem_limit_bytes=65400 * 1024
        ),
        name="moe_line",
    )(tokens, meta, expert_gate, expert_up, expert_down, shared_in, shared_down)


def choose(tokens, choices, affinity, expert_gate, *rest):
    tok = tokens.shape[0]
    ns, nt = lax.axis_size("expert"), lax.axis_size("tensor")
    piece = min(FFE, expert_gate.shape[1])
    fits = ns % 2 == 0 and piece % (128 * nt) == 0 and tok % (16 * nt) == 0 and expert_gate.shape[1] % piece == 0
    which = line_local if fits else local
    return which(tokens, choices, affinity, expert_gate, *rest)


def solution(mesh):
    placed = (
        P(("groups", "expert"), "tensor"),
        P(("groups", "expert"), None),
        P(("groups", "expert"), None),
        P("tensor", "expert"),
        P("tensor", "expert"),
        P("expert", "tensor"),
        P(None, "expert", "tensor"),
        P("expert", "tensor"),
    )
    return jax.shard_map(
        choose,
        mesh=mesh,
        in_specs=placed,
        out_specs=P(("groups", "expert"), "tensor"),
        check_vma=False,
    )
```

```python
import functools

import jax
import jax.numpy as jnp
from jax import lax
from jax.experimental import pallas as pl
from jax.experimental.pallas import tpu as pltpu
from jax.sharding import PartitionSpec as P

FFE = 1024
CAP = 48
MESH = pl.DeviceIdType.MESH
F32 = jnp.float32
BF16 = jnp.bfloat16


def mm(a, b, ca=1, cb=0):
    return lax.dot_general(a, b, (((ca,), (cb,)), ((), ())), preferred_element_type=F32)


def ring_rows(tok, hops, hop, rightward):
    if hop < hops:
        return 0, tok
    return (0, tok // 2) if rightward else (tok // 2, tok // 2)


def layer(
    dims, tokens, meta, gate_hbm, up_hbm, down_hbm, sin_hbm, sdown_hbm, out,
    x_all, meta_all, gate_w, up_w, down_w, sin_w, sdown_w, rows_buf, comb,
    part, core_in, x_out, x_in, hid, s_part, s_core_in, s_x_out, s_x_in, s_hid,
    rs_out, rs_in,
    load_sem, gate_sem, up_sem, down_sem, meta_sem, ag_sem, core_sem, x_sem, hx_sem, hc_sem, rs_sem,
):
    ns, nx, local_count, piece, tok, cap, top = dims
    hops = ns // 2
    z, t = lax.axis_index("expert"), lax.axis_index("tensor")
    x, c = lax.div(t, 2), lax.rem(t, 2)
    peer_c = 1 - c
    peer_t = 2 * x + peer_c
    right, left = lax.rem(z + 1, ns), lax.rem(z + ns - 1, ns)
    slots = gate_w.shape[0]

    def zoff(k):
        return lax.rem(z + k + ns, ns)

    def remote(src, dst, sems, index, where):
        send = sems.at[(0,) + index]
        recv = sems.at[(1,) + index]
        return pltpu.make_async_remote_copy(
            src_ref=src, dst_ref=dst, send_sem=send, recv_sem=recv, device_id=where, device_id_type=MESH
        )

    own_tok = pltpu.make_async_copy(tokens, x_all.at[z], load_sem.at[0])
    own_meta = pltpu.make_async_copy(meta, meta_all.at[z], load_sem.at[1])
    own_tok.start()
    own_meta.start()
    barrier = pltpu.get_barrier_semaphore()
    for k in range(1, ns):
        pl.semaphore_signal(barrier, inc=1, device_id={"expert": zoff(k)}, device_id_type=MESH)
    for k in range(1, nx):
        pl.semaphore_signal(
            barrier, inc=1, device_id={"tensor": 2 * lax.rem(x + k, nx) + c}, device_id_type=MESH
        )
    pl.semaphore_signal(barrier, inc=1, device_id={"tensor": peer_t}, device_id_type=MESH)

    sin_load = pltpu.make_async_copy(sin_hbm, sin_w, load_sem.at[2])
    sdown_load = pltpu.make_async_copy(sdown_hbm, sdown_w, load_sem.at[3])
    sin_load.start()

    def cols(e):
        return pl.ds(e * piece, piece)

    gate_loads = [
        pltpu.make_async_copy(gate_hbm.at[:, cols(e)], gate_w.at[e % slots], gate_sem.at[e])
        for e in range(local_count)
    ]
    up_loads = [
        pltpu.make_async_copy(up_hbm.at[:, cols(e)], up_w.at[e % slots], up_sem.at[e])
        for e in range(local_count)
    ]
    down_loads = [
        pltpu.make_async_copy(down_hbm.at[cols(e), :], down_w.at[e], down_sem.at[e])
        for e in range(local_count)
    ]
    own_tok.wait()
    own_meta.wait()
    pl.semaphore_wait(barrier, (ns - 1) + (nx - 1) + 1)

    def ag_copy(hop, rightward):
        start, size = ring_rows(tok, hops, hop, rightward)
        block = zoff(1 - hop) if rightward else zoff(hop - 1)
        ref = x_all.at[block, pl.ds(start, size), :]
        where = {"expert": right if rightward else left}
        return remote(ref, ref, ag_sem, (0 if rightward else 1, hop - 1), where)

    ag = {(h, d): ag_copy(h, d) for h in range(1, hops + 1) for d in (True, False)}
    for d in (True, False):
        ag[1, d].start()
    meta_copies = []
    for k in range(1, ns):
        copy = remote(meta_all.at[z], meta_all.at[z], meta_sem, (k - 1,), {"expert": zoff(k)})
        copy.start()
        meta_copies.append(copy)
    for e in range(min(slots, local_count)):
        gate_loads[e].start()
        up_loads[e].start()
    for e in range(local_count):
        down_loads[e].start()
    sdown_load.start()

    tri = (
        lax.broadcasted_iota(jnp.int32, (tok, tok), 0) < lax.broadcasted_iota(jnp.int32, (tok, tok), 1)
    ).astype(F32).astype(BF16)
    slot_of = lax.broadcasted_iota(jnp.int32, (cap, tok), 0).astype(F32)
    mask_rows = -(-local_count // 8) * 8
    row_of = lax.broadcasted_iota(jnp.int32, (mask_rows, tok), 0)
    columns = local_count * piece

    def dispatch(s):
        info = meta_all[s]
        masks, weights = [], []
        mask_all = jnp.zeros((mask_rows, tok), F32)
        for l in range(local_count):
            eid = lax.div(z * columns + l * piece, FFE).astype(F32)
            hit = (info[:top] == eid).astype(F32)
            mask = jnp.sum(hit, axis=0, keepdims=True)
            masks.append(mask)
            weights.append(jnp.sum(hit * info[top : 2 * top], axis=0, keepdims=True))
            mask_all = jnp.where(row_of == l, mask, mask_all)
        position = mm(mask_all.astype(BF16), tri)
        picks = []
        for l in range(local_count):
            pick = jnp.where((slot_of == position[l : l + 1]) & (masks[l] > 0.5), 1.0, 0.0)
            picks.append(pick.astype(BF16))
            comb[s, pl.ds(l * cap, cap), :] = (pick * weights[l]).astype(BF16)
        stacked = jnp.concatenate(picks, axis=0) if local_count > 1 else picks[0]
        gathered = mm(stacked, x_all[s]).astype(BF16)
        for l in range(local_count):
            rows_buf[l, s] = gathered[l * cap : (l + 1) * cap]

    for copy in meta_copies:
        copy.wait()
    dispatch(z)
    for hop in range(1, hops + 1):
        for d in (True, False):
            ag[hop, d].wait()
            if hop < hops:
                ag[hop + 1, d].start()
        dispatch(zoff(-hop))
        if hop < hops:
            dispatch(zoff(hop))

    unit_count = local_count + 1

    def unit(u):
        if u == 0:
            return s_part, s_core_in, s_x_out, s_x_in, s_hid
        e = u - 1
        return part.at[e], core_in.at[e], x_out.at[e], x_in.at[e], hid.at[e]

    def first(u):
        p, ci, _, _, _ = unit(u)
        if u == 0:
            sin_load.wait()
            whole = x_all[...].reshape(ns * tok, x_all.shape[2])
            for g in range(2):
                p[g] = mm(whole, sin_w[g], 1, 1).astype(BF16)
        else:
            e = u - 1
            lhs = rows_buf[e].reshape(ns * cap, x_all.shape[2])
            gate_loads[e].wait()
            p[0] = mm(lhs, gate_w[e % slots]).astype(BF16)
            up_loads[e].wait()
            p[1] = mm(lhs, up_w[e % slots]).astype(BF16)
            if e + slots < local_count:
                gate_loads[e + slots].start()
                up_loads[e + slots].start()
        half = p.shape[1] // 2
        theirs = pl.ds(pl.multiple_of(peer_c * half, half), half)
        copy = remote(p.at[:, theirs, :], ci, core_sem, (u,), {"tensor": peer_t})
        copy.start()
        return copy

    def chunk(p, ci, which):
        half = p.shape[1] // 2
        q = half // nx
        mine = pl.ds(pl.multiple_of(c * half + which * q, q), q)
        there = pl.ds(pl.multiple_of(which * q, q), q)
        return [p[g, mine, :].astype(F32) + ci[g, there, :].astype(F32) for g in range(2)]

    def second(u, core_copy):
        p, ci, xo, xi, _ = unit(u)
        core_copy.wait()
        copies = []
        for k in range(1, nx):
            other = lax.rem(x + k, nx)
            sums = chunk(p, ci, other)
            for g in range(2):
                xo[k - 1, g] = sums[g].astype(BF16)
            copy = remote(xo.at[k - 1], xi.at[k - 1], x_sem, (u, k - 1), {"tensor": 2 * other + c})
            copy.start()
            copies.append(copy)
        return copies

    def hid_rows(h, which):
        half = h.shape[0] // 2
        q = half // nx
        return h.at[pl.ds(pl.multiple_of(c * half + which * q, q), q), :]

    def third(u, x_copies):
        p, ci, _, xi, h = unit(u)
        sums = chunk(p, ci, x)
        for k in range(1, nx):
            x_copies[k - 1].wait()
            for g in range(2):
                sums[g] = sums[g] + xi[k - 1, g].astype(F32)
        gate, up = sums
        value = (gate / (1.0 + jnp.exp(-gate)) * up).astype(BF16)
        ref = hid_rows(h, x)
        ref[...] = value
        x_sends = []
        for k in range(1, nx):
            where = {"tensor": 2 * lax.rem(x + k, nx) + c}
            copy = remote(ref, ref, hx_sem, (u, k - 1), where)
            copy.start()
            x_sends.append(copy)
        copy = remote(ref, ref, hc_sem, (u, 0), {"tensor": peer_t})
        copy.start()
        return x_sends, [copy]

    def fourth(u, x_sends, core_sends):
        h = unit(u)[4]
        for k in range(1, nx):
            x_sends[k - 1].wait()
            ref = hid_rows(h, lax.rem(x + nx - k, nx))
            copy = remote(ref, ref, hc_sem, (u, k), {"tensor": peer_t})
            copy.start()
            core_sends.append(copy)
        return core_sends

    def fifth(u, core_sends):
        for copy in core_sends:
            copy.wait()
        if u > 0:
            e = u - 1
            down_loads[e].wait()
            made = mm(hid[e], down_w[e]).astype(BF16)
            rows_buf[e] = made.reshape(ns, cap, made.shape[1])

    state = {}
    for u in range(unit_count + 1):
        if u < unit_count:
            state[u] = first(u)
        if u >= 1:
            state[u - 1] = second(u - 1, state[u - 1])
    for u in range(unit_count + 2):
        if u < unit_count:
            state[u] = third(u, state[u])
        if 1 <= u <= unit_count:
            state[u - 1] = fourth(u - 1, *state[u - 1])
        if u >= 2:
            fifth(u - 2, state[u - 2])

    sdown_load.wait()

    def partial(s):
        made = rows_buf[:, s].reshape(local_count * cap, x_all.shape[2])
        shared = s_hid[pl.ds(pl.multiple_of(s * tok, tok), tok), :]
        return mm(comb[s], made, 0, 0) + mm(shared, sdown_w[...])

    def rs_copy(hop, rightward):
        start, size = ring_rows(tok, hops, hop, rightward)
        d = 0 if rightward else 1
        span = pl.ds(start, size)
        where = {"expert": right if rightward else left}
        return remote(
            rs_out.at[d, hop - 1, span, :], rs_in.at[d, hop - 1, span, :], rs_sem, (d, hop - 1), where
        )

    def arrived(hop, rightward):
        start, size = ring_rows(tok, hops, hop, rightward)
        got = rs_in[0 if rightward else 1, hop - 1, pl.ds(start, size), :].astype(F32)
        if size == tok:
            return got
        fill = jnp.zeros((tok - size, got.shape[1]), F32)
        return jnp.concatenate([got, fill] if start == 0 else [fill, got], axis=0)

    rs = {(h, d): rs_copy(h, d) for h in range(1, hops + 1) for d in (True, False)}
    opposite = partial(zoff(hops)).astype(BF16)
    for d in (True, False):
        start, size = ring_rows(tok, hops, hops, d)
        rs_out[0 if d else 1, hops - 1, pl.ds(start, size), :] = opposite[start : start + size]
        rs[hops, d].start()
    for hop in range(hops - 1, 0, -1):
        for d in (True, False):
            value = partial(zoff(hop if d else -hop))
            rs[hop + 1, d].wait()
            rs_out[0 if d else 1, hop - 1] = (value + arrived(hop + 1, d)).astype(BF16)
            rs[hop, d].start()
    total = partial(z)
    for d in (True, False):
        rs[1, d].wait()
        total = total + arrived(1, d)
    out[...] = total.astype(BF16)


def line_layer(
    dims, tokens, choices, affinity, gate_hbm, up_hbm, down_hbm, sin_hbm, sdown_hbm, out,
    x_all, choice_v, affinity_v, out_v, meta_all, gate_w, up_w, down_w, sin_w, sdown_w, rows, made, comb,
    part, core_in, x_out, x_in, hid, s_part, s_core_in, s_x_out, s_x_in, s_hid, rs_in,
    load_sem, gate_sem, up_sem, down_sem, meta_sem, ag_sem, core_sem, x_sem, hx_sem, hc_sem, rs_sem, rs_half_sem, out_sem,
):
    ns, nx, local_count, piece, tok, cap, top, pieces, cw = dims
    width = x_all.shape[2]
    z, t = lax.axis_index("expert"), lax.axis_index("tensor")
    x, c = lax.div(t, 2), lax.rem(t, 2)
    peer_c = 1 - c
    peer_t = 2 * x + peer_c
    mir = lax.div(z, ns // 2)
    zeta = z + mir * (ns - 1 - 2 * z)
    above = z + 1 - 2 * mir
    below = z - 1 + 2 * mir
    spread = tok // pieces

    def phys(b):
        return b + mir * (ns - 1 - 2 * b)

    def zoff(k):
        return lax.rem(z + k + ns, ns)

    def remote(src, dst, sems, index, where):
        send = sems.at[(0,) + index]
        recv = sems.at[(1,) + index]
        return pltpu.make_async_remote_copy(
            src_ref=src, dst_ref=dst, send_sem=send, recv_sem=recv, device_id=where, device_id_type=MESH
        )

    own_tok = pltpu.make_async_copy(tokens, x_all.at[z], load_sem.at[0])
    own_choice = pltpu.make_async_copy(choices, choice_v, load_sem.at[1])
    own_affinity = pltpu.make_async_copy(affinity, affinity_v, load_sem.at[4])
    own_choice.start()
    own_affinity.start()
    own_tok.start()
    barrier = pltpu.get_barrier_semaphore()
    for k in range(1, ns):
        pl.semaphore_signal(barrier, inc=1, device_id={"expert": zoff(k)}, device_id_type=MESH)
    for k in range(1, nx):
        pl.semaphore_signal(
            barrier, inc=1, device_id={"tensor": 2 * lax.rem(x + k, nx) + c}, device_id_type=MESH
        )
    pl.semaphore_signal(barrier, inc=1, device_id={"tensor": peer_t}, device_id_type=MESH)

    sin_load = pltpu.make_async_copy(sin_hbm, sin_w, load_sem.at[2])
    sdown_load = pltpu.make_async_copy(sdown_hbm, sdown_w, load_sem.at[3])

    def cols(e):
        return pl.ds(e * piece, piece)

    gate_loads = [
        pltpu.make_async_copy(gate_hbm.at[:, cols(e)], gate_w.at[e], gate_sem.at[e]) for e in range(local_count)
    ]
    up_loads = [
        pltpu.make_async_copy(up_hbm.at[:, cols(e)], up_w.at[e], up_sem.at[e]) for e in range(local_count)
    ]
    down_loads = [
        pltpu.make_async_copy(down_hbm.at[cols(e), :], down_w.at[e], down_sem.at[e]) for e in range(local_count)
    ]
    queue = [load for pair in zip(gate_loads, up_loads) for load in pair] + [sin_load] + down_loads + [sdown_load]

    def load_next(count):
        for load in queue[:count]:
            load.start()
        del queue[:count]

    load_next(3)
    own_choice.wait()
    own_affinity.wait()
    sigmoids = jax.nn.sigmoid(affinity_v[...])
    mix = 2.5 * sigmoids / jnp.sum(sigmoids, axis=0, keepdims=True)
    meta_all[z, :top] = choice_v[...].astype(F32)
    meta_all[z, top:] = mix
    own_tok.wait()
    pl.semaphore_wait(barrier, (ns - 1) + (nx - 1) + 1)

    def ag_copy(upward, b, k, where):
        d = mir if upward else 1 - mir
        block = phys(b)
        ref = x_all.at[block, pl.ds(k * spread, spread), :]
        return remote(ref, ref, ag_sem, (block + d, k), {"expert": where})

    for k in range(pieces):
        ag_copy(True, zeta, k, above).start()

        @pl.when(zeta > 0)
        def _():
            ag_copy(False, zeta, k, below).start()

    meta_copies = []
    for k in range(1, ns):
        copy = remote(meta_all.at[z], meta_all.at[z], meta_sem, (k - 1,), {"expert": zoff(k)})
        copy.start()
        meta_copies.append(copy)

    def from_above(b, k):
        ag_copy(False, b, k, above).wait_recv()

        @pl.when(zeta > 0)
        def _():
            ag_copy(False, b, k, below).start()

    def from_below(b, k):
        ag_copy(True, b, k, above).wait_recv()
        ag_copy(True, b, k, above).start()

    def arrive(i, k):
        far = (i + 1) // 2
        if i % 2:
            @pl.when(2 * zeta >= i)
            def _():
                from_below(zeta - far, k)
                from_above(zeta + far, k)

        @pl.when(2 * zeta < i)
        def _():
            from_above(i, k)

    def step_block(i):
        if i == 0:
            return z
        near = lax.div(2 * zeta - i + ns, ns)
        side = zeta - (i + 1) // 2 if i % 2 else zeta + i // 2
        return phys(near * side + (1 - near) * i)

    tri = (
        lax.broadcasted_iota(jnp.int32, (tok, tok), 0) < lax.broadcasted_iota(jnp.int32, (tok, tok), 1)
    ).astype(F32).astype(BF16)
    slot_of = lax.broadcasted_iota(jnp.int32, (cap, tok), 0).astype(F32)
    mask_rows = -(-local_count // 8) * 8
    row_of = lax.broadcasted_iota(jnp.int32, (mask_rows, tok), 0)
    columns = local_count * piece

    def dispatch(s):
        info = meta_all[s]
        masks, weights = [], []
        mask_all = jnp.zeros((mask_rows, tok), F32)
        for l in range(local_count):
            eid = lax.div(z * columns + l * piece, FFE).astype(F32)
            hit = (info[:top] == eid).astype(F32)
            mask = jnp.sum(hit, axis=0, keepdims=True)
            masks.append(mask)
            weights.append(jnp.sum(hit * info[top : 2 * top], axis=0, keepdims=True))
            mask_all = jnp.where(row_of == l, mask, mask_all)
        position = mm(mask_all.astype(BF16), tri)
        picks = []
        for l in range(local_count):
            pick = jnp.where((slot_of == position[l : l + 1]) & (masks[l] > 0.5), 1.0, 0.0)
            picks.append(pick.astype(BF16))
            comb[s, pl.ds(l * cap, cap), :] = (pick * weights[l]).astype(BF16)
        stacked = jnp.concatenate(picks, axis=0) if local_count > 1 else picks[0]
        gathered = mm(stacked, x_all[s]).astype(BF16)
        for l in range(local_count):
            rows[l] = gathered[l * cap : (l + 1) * cap]

    units = local_count + 1

    def refs(i, u):
        if u == local_count:
            return (
                s_part.at[i % 2], s_core_in.at[i], s_x_out.at[i], s_x_in.at[i], s_hid.at[step_block(i)]
            )
        return part.at[i % 2, u], core_in.at[i, u], x_out.at[i, u], x_in.at[i, u], hid.at[u, i]

    def along(u, start, size, lead):
        step = pl.ds(pl.multiple_of(start, size), size)
        return lead + ((step, slice(None)) if u == local_count else (slice(None), step))

    def turn(i):
        return 1 + (i - 1) % 2 if i else 0

    def extent(u):
        return tok if u == local_count else piece

    def first(i, u):
        p, ci = refs(i, u)[:2]
        if u == local_count:
            if i == 0:
                sin_load.wait()
            block = x_all[step_block(i)]
            for g in range(2):
                p[g] = mm(block, sin_w[g], 1, 1).astype(BF16)
        else:
            e = u
            lhs = rows[e]
            if i == 0:
                gate_loads[e].wait()
                load_next(1)
            p[0] = mm(lhs, gate_w[e]).astype(BF16)
            if i == 0:
                up_loads[e].wait()
                load_next(1)
            p[1] = mm(lhs, up_w[e]).astype(BF16)
        half = extent(u) // 2
        theirs = along(u, peer_c * half, half, (slice(None),))
        copy = remote(p.at[theirs], ci, core_sem, (i % 2, u), {"tensor": peer_t})
        copy.start()
        return copy

    def chunk(i, u, which):
        p, ci = refs(i, u)[:2]
        half = extent(u) // 2
        q = half // nx
        sums = []
        for g in range(2):
            mine = p[along(u, c * half + which * q, q, (g,))].astype(F32)
            sums.append(mine + ci[along(u, which * q, q, (g,))].astype(F32))
        return sums

    def second(i, u, core_copy):
        _, _, xo, xi, _ = refs(i, u)
        core_copy.wait()
        copies = []
        for k in range(1, nx):
            other = lax.rem(x + k, nx)
            sums = chunk(i, u, other)
            for g in range(2):
                xo[k - 1, g] = sums[g].astype(BF16)
            copy = remote(xo.at[k - 1], xi.at[k - 1], x_sem, (i % 2, u, k - 1), {"tensor": 2 * other + c})
            copy.start()
            copies.append(copy)
        return copies

    def hid_part(i, u, which):
        half = extent(u) // 2
        q = half // nx
        return refs(i, u)[4].at[along(u, c * half + which * q, q, ())]

    def third(i, u, x_copies):
        xi = refs(i, u)[3]
        sums = chunk(i, u, x)
        for k in range(1, nx):
            x_copies[k - 1].wait()
            for g in range(2):
                sums[g] = sums[g] + xi[k - 1, g].astype(F32)
        gate, up = sums
        value = (gate / (1.0 + jnp.exp(-gate)) * up).astype(BF16)
        ref = hid_part(i, u, x)
        ref[...] = value
        x_sends = []
        for k in range(1, nx):
            where = {"tensor": 2 * lax.rem(x + k, nx) + c}
            copy = remote(ref, ref, hx_sem, (i % 2, u, k - 1), where)
            copy.start()
            x_sends.append(copy)
        copy = remote(ref, ref, hc_sem, (turn(i), u, 0), {"tensor": peer_t})
        copy.start()
        return x_sends, [copy]

    def fourth(i, u, x_sends, core_sends):
        for k in range(1, nx):
            x_sends[k - 1].wait()
            ref = hid_part(i, u, lax.rem(x + nx - k, nx))
            copy = remote(ref, ref, hc_sem, (turn(i), u, k), {"tensor": peer_t})
            copy.start()
            core_sends.append(copy)
        return core_sends

    def fifth(i, u):
        span = (0, 1) if i == 1 else (i,)
        for j in span:
            for copy in state[j, u]:
                copy.wait()
        if u == local_count:
            if i == 1:
                sdown_load.wait()
            return
        if i == 1:
            down_loads[u].wait()
        count = len(span)
        lhs = hid[u, pl.ds(span[0], count)].reshape(count * cap, piece)
        result = mm(lhs, down_w[u]).astype(BF16)
        for n, j in enumerate(span):
            made[step_block(j), pl.ds(u * cap, cap), :] = result[n * cap : (n + 1) * cap]

    parts = width // cw

    def contribution(b, k):
        span = pl.ds(k * cw, cw)
        return mm(comb[b], made[b, :, span], 0, 0) + mm(s_hid[b], sdown_w[:, span])

    half_rows = tok // 2

    def spans(end):
        return [pl.ds(0, half_rows), pl.ds(half_rows, half_rows)] if end else [pl.ds(0, tok)]

    def rs_copy(upward, b, k, h, end, where):
        d = mir if upward else 1 - mir
        block = phys(b)
        slot = block + 1 - d
        span = (spans(end)[h], pl.ds(k * cw, cw))
        sems, index = (rs_half_sem, (d, k)) if h else (rs_sem, (slot, k))
        return remote(x_all.at[(block,) + span], rs_in.at[(slot,) + span], sems, index, {"expert": where})

    def arrived(upward, b, k, h, end):
        rs_copy(upward, b, k, h, end, above).wait_recv()
        d = mir if upward else 1 - mir
        return rs_in[phys(b) + 1 - d, spans(end)[h], pl.ds(k * cw, cw)].astype(F32)

    early = min(3, parts)

    def originate(r, span):
        @pl.when(zeta == 0)
        def _():
            for k in span:
                x_all[phys(r), :, pl.ds(k * cw, cw)] = contribution(phys(r), k).astype(BF16)
                end = r + 1 == ns
                for h in range(len(spans(end))):
                    rs_copy(True, r, k, h, end, above).start()

    def relay(upward, b, k):
        value = contribution(phys(b), k)
        end = b + 1 == ns if upward else b == 0
        for h, side in enumerate(spans(end)):
            total = value[side.start : side.start + side.size] + arrived(upward, b, k, h, end)
            x_all[phys(b), side, pl.ds(k * cw, cw)] = total.astype(BF16)
            rs_copy(upward, b, k, h, end, above if upward else below).start()

    state = {}

    def run(name, i, u):
        if name == "A":
            state[i, u] = first(i, u)
        elif name == "B":
            state[i, u] = second(i, u, state[i, u])
        elif name == "C":
            state[i, u] = third(i, u, state[i, u])
        elif name == "D":
            state[i, u] = fourth(i, u, *state[i, u])
        else:
            fifth(i, u)

    def inner(i, k):
        if i < ns:
            pl.when(zeta > 0)(functools.partial(arrive, i, k))

    def outer(i, k):
        pl.when(zeta == 0)(functools.partial(arrive, i, k))

    last = units - 1
    for i in range(ns):
        if i == 1:
            outer(1, 0)
            arrive(1, 1)
            for copy in meta_copies:
                copy.wait()
        elif i > 1:
            outer(i, 0)
            outer(i, 1)
        dispatch(step_block(i))
        for u in range(units):
            run("A", i, u)
            if u > 0:
                run("B", i, u - 1)
            if i == 0:
                if u >= 2:
                    run("C", i, u - 2)
                if u == 2:
                    inner(1, 0)
            else:
                if u == 0:
                    inner(i + 1, 1)
                if i < 3 and u < 2:
                    for v in range(-(-len(late) // (2 - u))):
                        run("C", i - 1, late.pop(0))
                if i > 2 and u == 0:
                    for v in range(units - 2):
                        run("D", i - 1, v)
                    relays = [units - 2, last]
                elif u == 1 and i < 3:
                    run("D", i - 1, 0)
                    run("D", i - 1, 1)
                    relays = list(range(2, units))
                elif u >= 3 or (i > 2 and u > 0):
                    for v in range(-(-len(relays) // (units - u)) if i < 3 else 1):
                        if relays:
                            run("D", i - 1, relays.pop(0))
                if u >= 3:
                    run("C", i, u - 3)
        if i > 0:
            inner(i + 2, 0)
        if i == 0:
            load_next(len(queue))
            run("B", 0, last)
            late = [units - 2, last]
            continue
        rest = list(range(units - 3, last))
        if i == 1:
            run("B", i, last)
            late = rest + [last]
            if i + 1 < ns:
                continue
            rest = late
        else:
            for u in range(units):
                run("E", i - 1, u)
                if u == 0:
                    run("B", i, last)
                elif rest and u < last:
                    run("C", i, rest.pop(0))
            originate(i - 1, range(early if i + 1 == ns else parts))
            rest.append(last)
        if i + 1 < ns:
            for u in rest:
                run("C", i, u)
    for u in rest:
        run("C", ns - 1, u)
    for u in range(units):
        if u == last:
            run("E", ns - 1, u - 2)
        run("D", ns - 1, u)
        if 2 <= u < last:
            run("E", ns - 1, u - 2)
    run("E", ns - 1, last - 1)
    run("E", ns - 1, last)
    originate(ns - 1, range(parts))
    if ns > 2:
        originate(ns - 2, range(early, parts))

    @pl.when(zeta > 0)
    def _():
        for k in range(pieces):
            ag_copy(True, zeta, k, above).wait_send()
            ag_copy(False, zeta, k, below).wait_send()
            for b in range(ns):
                @pl.when(b < zeta)
                def _():
                    ag_copy(True, b, k, above).wait_send()

                @pl.when(b > zeta)
                def _():
                    ag_copy(False, b, k, below).wait_send()

    order = [(r, k) for r in range(2, ns - 2) for k in range(parts)]
    if ns > 3:
        order += [(ns - 2, k) for k in range(early)]
    order += [(ns - 1, k) for k in range(parts)]
    if ns > 3:
        order += [(ns - 2, k) for k in range(early, parts)]
    for n in range(len(order) + 2):
        if n < len(order):
            r, k = order[n]
            pl.when((zeta > 0) & (zeta < r))(functools.partial(relay, True, r, k))
        if n >= 2:
            r, k = order[n - 2]
            if r > ns // 2:
                pl.when(zeta > ns - 1 - r)(functools.partial(relay, False, ns - 1 - r, k))

    def finish(inside):
        for k in range(parts):
            span = pl.ds(k * cw, cw)
            value = contribution(z, k)
            for h, side in enumerate(spans(not inside)):
                total = value[side.start : side.start + side.size] + arrived(False, zeta, k, h, not inside)
                if inside:
                    total = total + arrived(True, zeta, k, h, False)
                out_v[side, span] = total.astype(BF16)
            pltpu.make_async_copy(out_v.at[:, span], out.at[:, span], out_sem).start()

    pl.when(zeta == 0)(functools.partial(finish, False))
    pl.when(zeta > 0)(functools.partial(finish, True))

    @pl.when(zeta == 0)
    def _():
        for k in range(pieces):
            ag_copy(True, zeta, k, above).wait_send()

    def sent(upward, b):
        end = b + 1 == ns if upward else b == 0
        for k in range(parts):
            for h in range(len(spans(end))):
                rs_copy(upward, b, k, h, end, above).wait_send()

    for b in range(ns):
        pl.when(zeta < b)(functools.partial(sent, True, b))
        pl.when(zeta > b)(functools.partial(sent, False, b))
    pltpu.make_async_copy(out_v, out, out_sem).wait()


def local(tokens, choices, affinity, expert_gate, expert_up, expert_down, shared_in, shared_down):
    tok, width = tokens.shape
    top = choices.shape[1]
    ns, nt = lax.axis_size("expert"), lax.axis_size("tensor")
    nx = nt // 2
    piece = min(FFE, expert_gate.shape[1])
    local_count = expert_gate.shape[1] // piece
    hs = shared_in.shape[1]
    hops = ns // 2
    slots = min(3, local_count)
    sigmoids = jax.nn.sigmoid(affinity)
    mix = 2.5 * sigmoids / jnp.sum(sigmoids, axis=1, keepdims=True)
    meta = jnp.concatenate([choices.astype(F32).T, mix.T], axis=0)
    rows = ns * CAP
    srows = ns * tok
    units = local_count + 1
    dims = (ns, nx, local_count, piece, tok, CAP, top)
    hbm = pl.BlockSpec(memory_space=pl.ANY)
    sem = pltpu.SemaphoreType.DMA
    scratch = [
        pltpu.VMEM((ns, tok, width), BF16),
        pltpu.VMEM((ns,) + meta.shape, F32),
        pltpu.VMEM((slots, width, piece), BF16),
        pltpu.VMEM((slots, width, piece), BF16),
        pltpu.VMEM((local_count, piece, width), BF16),
        pltpu.VMEM(shared_in.shape, BF16),
        pltpu.VMEM(shared_down.shape, BF16),
        pltpu.VMEM((local_count, ns, CAP, width), BF16),
        pltpu.VMEM((ns, local_count * CAP, tok), BF16),
        pltpu.VMEM((local_count, 2, rows, piece), BF16),
        pltpu.VMEM((local_count, 2, rows // 2, piece), BF16),
        pltpu.VMEM((local_count, nx - 1, 2, rows // nt, piece), BF16),
        pltpu.VMEM((local_count, nx - 1, 2, rows // nt, piece), BF16),
        pltpu.VMEM((local_count, rows, piece), BF16),
        pltpu.VMEM((2, srows, hs), BF16),
        pltpu.VMEM((2, srows // 2, hs), BF16),
        pltpu.VMEM((nx - 1, 2, srows // nt, hs), BF16),
        pltpu.VMEM((nx - 1, 2, srows // nt, hs), BF16),
        pltpu.VMEM((srows, hs), BF16),
        pltpu.VMEM((2, hops, tok, width), BF16),
        pltpu.VMEM((2, hops, tok, width), BF16),
        sem((4,)),
        sem((local_count,)),
        sem((local_count,)),
        sem((local_count,)),
        sem((2, ns - 1)),
        sem((2, 2, hops)),
        sem((2, units)),
        sem((2, units, nx - 1)),
        sem((2, units, nx - 1)),
        sem((2, units, nx)),
        sem((2, 2, hops)),
    ]
    return pl.pallas_call(
        functools.partial(layer, dims),
        out_shape=jax.ShapeDtypeStruct((tok, width), BF16),
        in_specs=[hbm] * 7,
        out_specs=pl.BlockSpec(memory_space=pltpu.VMEM),
        scratch_shapes=scratch,
        compiler_params=pltpu.CompilerParams(
            collective_id=0, has_side_effects=True, vmem_limit_bytes=60 * 1024 * 1024
        ),
        name="moe_layer",
    )(tokens, meta, expert_gate, expert_up, expert_down, shared_in, shared_down)


def line_local(tokens, choices, affinity, expert_gate, expert_up, expert_down, shared_in, shared_down):
    tok, width = tokens.shape
    top = choices.shape[1]
    ns, nt = lax.axis_size("expert"), lax.axis_size("tensor")
    nx = nt // 2
    piece = min(FFE, expert_gate.shape[1])
    local_count = expert_gate.shape[1] // piece
    hs = shared_in.shape[1]
    pieces = 2
    cw = 256 if width % 256 == 0 else 128
    units = local_count + 1
    dims = (ns, nx, local_count, piece, tok, CAP, top, pieces, cw)
    hbm = pl.BlockSpec(memory_space=pl.ANY)
    sem = pltpu.SemaphoreType.DMA
    scratch = [
        pltpu.VMEM((ns, tok, width), BF16),
        pltpu.VMEM((top, tok), jnp.int32),
        pltpu.VMEM((top, tok), F32),
        pltpu.VMEM((tok, width), BF16),
        pltpu.VMEM((ns, 2 * top, tok), F32),
        pltpu.VMEM((local_count, width, piece), BF16),
        pltpu.VMEM((local_count, width, piece), BF16),
        pltpu.VMEM((local_count, piece, width), BF16),
        pltpu.VMEM(shared_in.shape, BF16),
        pltpu.VMEM(shared_down.shape, BF16),
        pltpu.VMEM((local_count, CAP, width), BF16),
        pltpu.VMEM((ns, local_count * CAP, width), BF16),
        pltpu.VMEM((ns, local_count * CAP, tok), BF16),
        pltpu.VMEM((2, local_count, 2, CAP, piece), BF16),
        pltpu.VMEM((ns, local_count, 2, CAP, piece // 2), BF16),
        pltpu.VMEM((ns, local_count, nx - 1, 2, CAP, piece // nt), BF16),
        pltpu.VMEM((ns, local_count, nx - 1, 2, CAP, piece // nt), BF16),
        pltpu.VMEM((local_count, ns, CAP, piece), BF16),
        pltpu.VMEM((2, 2, tok, hs), BF16),
        pltpu.VMEM((ns, 2, tok // 2, hs), BF16),
        pltpu.VMEM((ns, nx - 1, 2, tok // nt, hs), BF16),
        pltpu.VMEM((ns, nx - 1, 2, tok // nt, hs), BF16),
        pltpu.VMEM((ns, tok, hs), BF16),
        pltpu.VMEM((ns + 1, tok, width), BF16),
        sem((5,)),
        sem((local_count,)),
        sem((local_count,)),
        sem((local_count,)),
        sem((2, ns - 1)),
        sem((2, ns + 1, pieces)),
        sem((2, 2, units)),
        sem((2, 2, units, nx - 1)),
        sem((2, 2, units, nx - 1)),
        sem((2, 3, units, nx)),
        sem((2, ns + 1, width // cw)),
        sem((2, 2, width // cw)),
        sem(()),
    ]
    return pl.pallas_call(
        functools.partial(line_layer, dims),
        out_shape=jax.ShapeDtypeStruct((tok, width), BF16),
        in_specs=[hbm] * 8,
        out_specs=hbm,
        scratch_shapes=scratch,
        compiler_params=pltpu.CompilerParams(
            collective_id=0, has_side_effects=True, vmem_limit_bytes=65400 * 1024
        ),
        name="moe_line",
    )(tokens, choices.T, affinity.T, expert_gate, expert_up, expert_down, shared_in, shared_down)


def choose(tokens, choices, affinity, expert_gate, *rest):
    tok = tokens.shape[0]
    ns, nt = lax.axis_size("expert"), lax.axis_size("tensor")
    piece = min(FFE, expert_gate.shape[1])
    fits = ns % 2 == 0 and piece % (128 * nt) == 0 and tok % (16 * nt) == 0 and expert_gate.shape[1] % piece == 0
    which = line_local if fits else local
    return which(tokens, choices, affinity, expert_gate, *rest)


def solution(mesh):
    placed = (
        P(("groups", "expert"), "tensor"),
        P(("groups", "expert"), None),
        P(("groups", "expert"), None),
        P("tensor", "expert"),
        P("tensor", "expert"),
        P("expert", "tensor"),
        P(None, "expert", "tensor"),
        P("expert", "tensor"),
    )
    return jax.shard_map(
        choose,
        mesh=mesh,
        in_specs=placed,
        out_specs=P(("groups", "expert"), "tensor"),
        check_vma=False,
    )
```

```python
import functools

import jax
import jax.numpy as jnp
from jax import lax
from jax.experimental import pallas as pl
from jax.experimental.pallas import tpu as pltpu
from jax.sharding import PartitionSpec as P

FFE = 1024
CAP = 48
MESH = pl.DeviceIdType.MESH
F32 = jnp.float32
BF16 = jnp.bfloat16


def mm(a, b, ca=1, cb=0):
    return lax.dot_general(a, b, (((ca,), (cb,)), ((), ())), preferred_element_type=F32)


def ring_rows(tok, hops, hop, rightward):
    if hop < hops:
        return 0, tok
    return (0, tok // 2) if rightward else (tok // 2, tok // 2)


def layer(
    dims, tokens, meta, gate_hbm, up_hbm, down_hbm, sin_hbm, sdown_hbm, out,
    x_all, meta_all, gate_w, up_w, down_w, sin_w, sdown_w, rows_buf, comb,
    part, core_in, x_out, x_in, hid, s_part, s_core_in, s_x_out, s_x_in, s_hid,
    rs_out, rs_in,
    load_sem, gate_sem, up_sem, down_sem, meta_sem, ag_sem, core_sem, x_sem, hx_sem, hc_sem, rs_sem,
):
    ns, nx, local_count, piece, tok, cap, top = dims
    hops = ns // 2
    z, t = lax.axis_index("expert"), lax.axis_index("tensor")
    x, c = lax.div(t, 2), lax.rem(t, 2)
    peer_c = 1 - c
    peer_t = 2 * x + peer_c
    right, left = lax.rem(z + 1, ns), lax.rem(z + ns - 1, ns)
    slots = gate_w.shape[0]

    def zoff(k):
        return lax.rem(z + k + ns, ns)

    def remote(src, dst, sems, index, where):
        send = sems.at[(0,) + index]
        recv = sems.at[(1,) + index]
        return pltpu.make_async_remote_copy(
            src_ref=src, dst_ref=dst, send_sem=send, recv_sem=recv, device_id=where, device_id_type=MESH
        )

    own_tok = pltpu.make_async_copy(tokens, x_all.at[z], load_sem.at[0])
    own_meta = pltpu.make_async_copy(meta, meta_all.at[z], load_sem.at[1])
    own_tok.start()
    own_meta.start()
    barrier = pltpu.get_barrier_semaphore()
    for k in range(1, ns):
        pl.semaphore_signal(barrier, inc=1, device_id={"expert": zoff(k)}, device_id_type=MESH)
    for k in range(1, nx):
        pl.semaphore_signal(
            barrier, inc=1, device_id={"tensor": 2 * lax.rem(x + k, nx) + c}, device_id_type=MESH
        )
    pl.semaphore_signal(barrier, inc=1, device_id={"tensor": peer_t}, device_id_type=MESH)

    sin_load = pltpu.make_async_copy(sin_hbm, sin_w, load_sem.at[2])
    sdown_load = pltpu.make_async_copy(sdown_hbm, sdown_w, load_sem.at[3])
    sin_load.start()

    def cols(e):
        return pl.ds(e * piece, piece)

    gate_loads = [
        pltpu.make_async_copy(gate_hbm.at[:, cols(e)], gate_w.at[e % slots], gate_sem.at[e])
        for e in range(local_count)
    ]
    up_loads = [
        pltpu.make_async_copy(up_hbm.at[:, cols(e)], up_w.at[e % slots], up_sem.at[e])
        for e in range(local_count)
    ]
    down_loads = [
        pltpu.make_async_copy(down_hbm.at[cols(e), :], down_w.at[e], down_sem.at[e])
        for e in range(local_count)
    ]
    own_tok.wait()
    own_meta.wait()
    pl.semaphore_wait(barrier, (ns - 1) + (nx - 1) + 1)

    def ag_copy(hop, rightward):
        start, size = ring_rows(tok, hops, hop, rightward)
        block = zoff(1 - hop) if rightward else zoff(hop - 1)
        ref = x_all.at[block, pl.ds(start, size), :]
        where = {"expert": right if rightward else left}
        return remote(ref, ref, ag_sem, (0 if rightward else 1, hop - 1), where)

    ag = {(h, d): ag_copy(h, d) for h in range(1, hops + 1) for d in (True, False)}
    for d in (True, False):
        ag[1, d].start()
    meta_copies = []
    for k in range(1, ns):
        copy = remote(meta_all.at[z], meta_all.at[z], meta_sem, (k - 1,), {"expert": zoff(k)})
        copy.start()
        meta_copies.append(copy)
    for e in range(min(slots, local_count)):
        gate_loads[e].start()
        up_loads[e].start()
    for e in range(local_count):
        down_loads[e].start()
    sdown_load.start()

    tri = (
        lax.broadcasted_iota(jnp.int32, (tok, tok), 0) < lax.broadcasted_iota(jnp.int32, (tok, tok), 1)
    ).astype(F32).astype(BF16)
    slot_of = lax.broadcasted_iota(jnp.int32, (cap, tok), 0).astype(F32)
    mask_rows = -(-local_count // 8) * 8
    row_of = lax.broadcasted_iota(jnp.int32, (mask_rows, tok), 0)
    columns = local_count * piece

    def dispatch(s):
        info = meta_all[s]
        masks, weights = [], []
        mask_all = jnp.zeros((mask_rows, tok), F32)
        for l in range(local_count):
            eid = lax.div(z * columns + l * piece, FFE).astype(F32)
            hit = (info[:top] == eid).astype(F32)
            mask = jnp.sum(hit, axis=0, keepdims=True)
            masks.append(mask)
            weights.append(jnp.sum(hit * info[top : 2 * top], axis=0, keepdims=True))
            mask_all = jnp.where(row_of == l, mask, mask_all)
        position = mm(mask_all.astype(BF16), tri)
        picks = []
        for l in range(local_count):
            pick = jnp.where((slot_of == position[l : l + 1]) & (masks[l] > 0.5), 1.0, 0.0)
            picks.append(pick.astype(BF16))
            comb[s, pl.ds(l * cap, cap), :] = (pick * weights[l]).astype(BF16)
        stacked = jnp.concatenate(picks, axis=0) if local_count > 1 else picks[0]
        gathered = mm(stacked, x_all[s]).astype(BF16)
        for l in range(local_count):
            rows_buf[l, s] = gathered[l * cap : (l + 1) * cap]

    for copy in meta_copies:
        copy.wait()
    dispatch(z)
    for hop in range(1, hops + 1):
        for d in (True, False):
            ag[hop, d].wait()
            if hop < hops:
                ag[hop + 1, d].start()
        dispatch(zoff(-hop))
        if hop < hops:
            dispatch(zoff(hop))

    unit_count = local_count + 1

    def unit(u):
        if u == 0:
            return s_part, s_core_in, s_x_out, s_x_in, s_hid
        e = u - 1
        return part.at[e], core_in.at[e], x_out.at[e], x_in.at[e], hid.at[e]

    def first(u):
        p, ci, _, _, _ = unit(u)
        if u == 0:
            sin_load.wait()
            whole = x_all[...].reshape(ns * tok, x_all.shape[2])
            for g in range(2):
                p[g] = mm(whole, sin_w[g], 1, 1).astype(BF16)
        else:
            e = u - 1
            lhs = rows_buf[e].reshape(ns * cap, x_all.shape[2])
            gate_loads[e].wait()
            p[0] = mm(lhs, gate_w[e % slots]).astype(BF16)
            up_loads[e].wait()
            p[1] = mm(lhs, up_w[e % slots]).astype(BF16)
            if e + slots < local_count:
                gate_loads[e + slots].start()
                up_loads[e + slots].start()
        half = p.shape[1] // 2
        theirs = pl.ds(pl.multiple_of(peer_c * half, half), half)
        copy = remote(p.at[:, theirs, :], ci, core_sem, (u,), {"tensor": peer_t})
        copy.start()
        return copy

    def chunk(p, ci, which):
        half = p.shape[1] // 2
        q = half // nx
        mine = pl.ds(pl.multiple_of(c * half + which * q, q), q)
        there = pl.ds(pl.multiple_of(which * q, q), q)
        return [p[g, mine, :].astype(F32) + ci[g, there, :].astype(F32) for g in range(2)]

    def second(u, core_copy):
        p, ci, xo, xi, _ = unit(u)
        core_copy.wait()
        copies = []
        for k in range(1, nx):
            other = lax.rem(x + k, nx)
            sums = chunk(p, ci, other)
            for g in range(2):
                xo[k - 1, g] = sums[g].astype(BF16)
            copy = remote(xo.at[k - 1], xi.at[k - 1], x_sem, (u, k - 1), {"tensor": 2 * other + c})
            copy.start()
            copies.append(copy)
        return copies

    def hid_rows(h, which):
        half = h.shape[0] // 2
        q = half // nx
        return h.at[pl.ds(pl.multiple_of(c * half + which * q, q), q), :]

    def third(u, x_copies):
        p, ci, _, xi, h = unit(u)
        sums = chunk(p, ci, x)
        for k in range(1, nx):
            x_copies[k - 1].wait()
            for g in range(2):
                sums[g] = sums[g] + xi[k - 1, g].astype(F32)
        gate, up = sums
        value = (gate / (1.0 + jnp.exp(-gate)) * up).astype(BF16)
        ref = hid_rows(h, x)
        ref[...] = value
        x_sends = []
        for k in range(1, nx):
            where = {"tensor": 2 * lax.rem(x + k, nx) + c}
            copy = remote(ref, ref, hx_sem, (u, k - 1), where)
            copy.start()
            x_sends.append(copy)
        copy = remote(ref, ref, hc_sem, (u, 0), {"tensor": peer_t})
        copy.start()
        return x_sends, [copy]

    def fourth(u, x_sends, core_sends):
        h = unit(u)[4]
        for k in range(1, nx):
            x_sends[k - 1].wait()
            ref = hid_rows(h, lax.rem(x + nx - k, nx))
            copy = remote(ref, ref, hc_sem, (u, k), {"tensor": peer_t})
            copy.start()
            core_sends.append(copy)
        return core_sends

    def fifth(u, core_sends):
        for copy in core_sends:
            copy.wait()
        if u > 0:
            e = u - 1
            down_loads[e].wait()
            made = mm(hid[e], down_w[e]).astype(BF16)
            rows_buf[e] = made.reshape(ns, cap, made.shape[1])

    state = {}
    for u in range(unit_count + 1):
        if u < unit_count:
            state[u] = first(u)
        if u >= 1:
            state[u - 1] = second(u - 1, state[u - 1])
    for u in range(unit_count + 2):
        if u < unit_count:
            state[u] = third(u, state[u])
        if 1 <= u <= unit_count:
            state[u - 1] = fourth(u - 1, *state[u - 1])
        if u >= 2:
            fifth(u - 2, state[u - 2])

    sdown_load.wait()

    def partial(s):
        made = rows_buf[:, s].reshape(local_count * cap, x_all.shape[2])
        shared = s_hid[pl.ds(pl.multiple_of(s * tok, tok), tok), :]
        return mm(comb[s], made, 0, 0) + mm(shared, sdown_w[...])

    def rs_copy(hop, rightward):
        start, size = ring_rows(tok, hops, hop, rightward)
        d = 0 if rightward else 1
        span = pl.ds(start, size)
        where = {"expert": right if rightward else left}
        return remote(
            rs_out.at[d, hop - 1, span, :], rs_in.at[d, hop - 1, span, :], rs_sem, (d, hop - 1), where
        )

    def arrived(hop, rightward):
        start, size = ring_rows(tok, hops, hop, rightward)
        got = rs_in[0 if rightward else 1, hop - 1, pl.ds(start, size), :].astype(F32)
        if size == tok:
            return got
        fill = jnp.zeros((tok - size, got.shape[1]), F32)
        return jnp.concatenate([got, fill] if start == 0 else [fill, got], axis=0)

    rs = {(h, d): rs_copy(h, d) for h in range(1, hops + 1) for d in (True, False)}
    opposite = partial(zoff(hops)).astype(BF16)
    for d in (True, False):
        start, size = ring_rows(tok, hops, hops, d)
        rs_out[0 if d else 1, hops - 1, pl.ds(start, size), :] = opposite[start : start + size]
        rs[hops, d].start()
    for hop in range(hops - 1, 0, -1):
        for d in (True, False):
            value = partial(zoff(hop if d else -hop))
            rs[hop + 1, d].wait()
            rs_out[0 if d else 1, hop - 1] = (value + arrived(hop + 1, d)).astype(BF16)
            rs[hop, d].start()
    total = partial(z)
    for d in (True, False):
        rs[1, d].wait()
        total = total + arrived(1, d)
    out[...] = total.astype(BF16)


def line_layer(
    dims, tokens, choices, affinity, gate_hbm, up_hbm, down_hbm, sin_hbm, sdown_hbm, out,
    x_all, choice_v, affinity_v, out_v, meta_all, gate_w, up_w, down_w, sin_w, sdown_w, rows, made, comb,
    part, core_in, x_out, x_in, hid, s_part, s_core_in, s_x_out, s_x_in, s_hid, rs_in,
    load_sem, gate_sem, up_sem, down_sem, meta_sem, ag_sem, core_sem, x_sem, hx_sem, hc_sem, rs_sem, rs_half_sem, out_sem,
):
    ns, nx, local_count, piece, tok, cap, top, pieces, cw = dims
    width = x_all.shape[2]
    z, t = lax.axis_index("expert"), lax.axis_index("tensor")
    x, c = lax.div(t, 2), lax.rem(t, 2)
    peer_c = 1 - c
    peer_t = 2 * x + peer_c
    mir = lax.div(z, ns // 2)
    zeta = z + mir * (ns - 1 - 2 * z)
    above = z + 1 - 2 * mir
    below = z - 1 + 2 * mir
    spread = tok // pieces

    def phys(b):
        return b + mir * (ns - 1 - 2 * b)

    def zoff(k):
        return lax.rem(z + k + ns, ns)

    def remote(src, dst, sems, index, where):
        send = sems.at[(0,) + index]
        recv = sems.at[(1,) + index]
        return pltpu.make_async_remote_copy(
            src_ref=src, dst_ref=dst, send_sem=send, recv_sem=recv, device_id=where, device_id_type=MESH
        )

    own_tok = pltpu.make_async_copy(tokens, x_all.at[z], load_sem.at[0])
    own_choice = pltpu.make_async_copy(choices, choice_v, load_sem.at[1])
    own_affinity = pltpu.make_async_copy(affinity, affinity_v, load_sem.at[4])
    own_choice.start()
    own_affinity.start()
    own_tok.start()
    barrier = pltpu.get_barrier_semaphore()
    for k in range(1, ns):
        pl.semaphore_signal(barrier, inc=1, device_id={"expert": zoff(k)}, device_id_type=MESH)
    for k in range(1, nx):
        pl.semaphore_signal(
            barrier, inc=1, device_id={"tensor": 2 * lax.rem(x + k, nx) + c}, device_id_type=MESH
        )
    pl.semaphore_signal(barrier, inc=1, device_id={"tensor": peer_t}, device_id_type=MESH)

    sin_load = pltpu.make_async_copy(sin_hbm, sin_w, load_sem.at[2])
    sdown_load = pltpu.make_async_copy(sdown_hbm, sdown_w, load_sem.at[3])

    def cols(e):
        return pl.ds(e * piece, piece)

    gate_loads = [
        pltpu.make_async_copy(gate_hbm.at[:, cols(e)], gate_w.at[e], gate_sem.at[e]) for e in range(local_count)
    ]
    up_loads = [
        pltpu.make_async_copy(up_hbm.at[:, cols(e)], up_w.at[e], up_sem.at[e]) for e in range(local_count)
    ]
    down_loads = [
        pltpu.make_async_copy(down_hbm.at[cols(e), :], down_w.at[e], down_sem.at[e]) for e in range(local_count)
    ]
    queue = [load for pair in zip(gate_loads, up_loads) for load in pair] + [sin_load] + down_loads + [sdown_load]

    def load_next(count):
        for load in queue[:count]:
            load.start()
        del queue[:count]

    load_next(3)
    own_choice.wait()
    own_affinity.wait()
    sigmoids = jax.nn.sigmoid(affinity_v[...])
    mix = 2.5 * sigmoids / jnp.sum(sigmoids, axis=0, keepdims=True)
    meta_all[z, :top] = choice_v[...].astype(F32)
    meta_all[z, top:] = mix
    own_tok.wait()
    pl.semaphore_wait(barrier, (ns - 1) + (nx - 1) + 1)

    def ag_copy(upward, b, k, where):
        d = mir if upward else 1 - mir
        block = phys(b)
        ref = x_all.at[block, pl.ds(k * spread, spread), :]
        return remote(ref, ref, ag_sem, (block + d, k), {"expert": where})

    for k in range(pieces):
        ag_copy(True, zeta, k, above).start()

        @pl.when(zeta > 0)
        def _():
            ag_copy(False, zeta, k, below).start()

    meta_copies = []
    for k in range(1, ns):
        copy = remote(meta_all.at[z], meta_all.at[z], meta_sem, (k - 1,), {"expert": zoff(k)})
        copy.start()
        meta_copies.append(copy)

    def from_above(b, k):
        ag_copy(False, b, k, above).wait_recv()

        @pl.when(zeta > 0)
        def _():
            ag_copy(False, b, k, below).start()

    def from_below(b, k):
        ag_copy(True, b, k, above).wait_recv()
        ag_copy(True, b, k, above).start()

    def arrive(i, k):
        far = (i + 1) // 2
        if i % 2:
            @pl.when(2 * zeta >= i)
            def _():
                from_below(zeta - far, k)
                from_above(zeta + far, k)

        @pl.when(2 * zeta < i)
        def _():
            from_above(i, k)

    def step_block(i):
        if i == 0:
            return z
        near = lax.div(2 * zeta - i + ns, ns)
        side = zeta - (i + 1) // 2 if i % 2 else zeta + i // 2
        return phys(near * side + (1 - near) * i)

    tri = (
        lax.broadcasted_iota(jnp.int32, (tok, tok), 0) < lax.broadcasted_iota(jnp.int32, (tok, tok), 1)
    ).astype(F32).astype(BF16)
    slot_of = lax.broadcasted_iota(jnp.int32, (cap, tok), 0).astype(F32)
    mask_rows = -(-local_count // 8) * 8
    row_of = lax.broadcasted_iota(jnp.int32, (mask_rows, tok), 0)
    columns = local_count * piece

    def dispatch(s):
        info = meta_all[s]
        masks, weights = [], []
        mask_all = jnp.zeros((mask_rows, tok), F32)
        for l in range(local_count):
            eid = lax.div(z * columns + l * piece, FFE).astype(F32)
            hit = (info[:top] == eid).astype(F32)
            mask = jnp.sum(hit, axis=0, keepdims=True)
            masks.append(mask)
            weights.append(jnp.sum(hit * info[top : 2 * top], axis=0, keepdims=True))
            mask_all = jnp.where(row_of == l, mask, mask_all)
        position = mm(mask_all.astype(BF16), tri)
        picks = []
        for l in range(local_count):
            pick = jnp.where((slot_of == position[l : l + 1]) & (masks[l] > 0.5), 1.0, 0.0)
            picks.append(pick.astype(BF16))
            comb[s, pl.ds(l * cap, cap), :] = (pick * weights[l]).astype(BF16)
        stacked = jnp.concatenate(picks, axis=0) if local_count > 1 else picks[0]
        gathered = mm(stacked, x_all[s]).astype(BF16)
        for l in range(local_count):
            rows[l] = gathered[l * cap : (l + 1) * cap]

    units = local_count + 1

    def refs(i, u):
        if u == local_count:
            return (
                s_part.at[i % 2], s_core_in.at[i], s_x_out.at[i], s_x_in.at[i], s_hid.at[step_block(i)]
            )
        return part.at[i % 2, u], core_in.at[i, u], x_out.at[i, u], x_in.at[i, u], hid.at[u, i]

    def along(u, start, size, lead):
        step = pl.ds(pl.multiple_of(start, size), size)
        return lead + ((step, slice(None)) if u == local_count else (slice(None), step))

    def turn(i):
        return 1 + (i - 1) % 2 if i else 0

    def extent(u):
        return tok if u == local_count else piece

    def first(i, u):
        p, ci = refs(i, u)[:2]
        if u == local_count:
            if i == 0:
                sin_load.wait()
            block = x_all[step_block(i)]
            for g in range(2):
                p[g] = mm(block, sin_w[g], 1, 1).astype(BF16)
        else:
            e = u
            first_row = e if e + 1 < local_count else max(e - 1, 0)
            pair = min(2, local_count)
            lhs = rows[first_row : first_row + pair].reshape(pair * cap, width)
            keep = slice((e - first_row) * cap, (e - first_row + 1) * cap)
            if i == 0:
                gate_loads[e].wait()
                load_next(1)
            p[0] = mm(lhs, gate_w[e])[keep].astype(BF16)
            if i == 0:
                up_loads[e].wait()
                load_next(1)
            p[1] = mm(lhs, up_w[e])[keep].astype(BF16)
        half = extent(u) // 2
        theirs = along(u, peer_c * half, half, (slice(None),))
        copy = remote(p.at[theirs], ci, core_sem, (i % 2, u), {"tensor": peer_t})
        copy.start()
        return copy

    def chunk(i, u, which):
        p, ci = refs(i, u)[:2]
        half = extent(u) // 2
        q = half // nx
        sums = []
        for g in range(2):
            mine = p[along(u, c * half + which * q, q, (g,))].astype(F32)
            sums.append(mine + ci[along(u, which * q, q, (g,))].astype(F32))
        return sums

    def second(i, u, core_copy):
        _, _, xo, xi, _ = refs(i, u)
        core_copy.wait()
        copies = []
        for k in range(1, nx):
            other = lax.rem(x + k, nx)
            sums = chunk(i, u, other)
            for g in range(2):
                xo[k - 1, g] = sums[g].astype(BF16)
            copy = remote(xo.at[k - 1], xi.at[k - 1], x_sem, (i % 2, u, k - 1), {"tensor": 2 * other + c})
            copy.start()
            copies.append(copy)
        return copies

    def hid_part(i, u, which):
        half = extent(u) // 2
        q = half // nx
        return refs(i, u)[4].at[along(u, c * half + which * q, q, ())]

    def third(i, u, x_copies):
        xi = refs(i, u)[3]
        sums = chunk(i, u, x)
        for k in range(1, nx):
            x_copies[k - 1].wait()
            for g in range(2):
                sums[g] = sums[g] + xi[k - 1, g].astype(F32)
        gate, up = sums
        value = (gate / (1.0 + jnp.exp(-gate)) * up).astype(BF16)
        ref = hid_part(i, u, x)
        ref[...] = value
        x_sends = []
        for k in range(1, nx):
            where = {"tensor": 2 * lax.rem(x + k, nx) + c}
            copy = remote(ref, ref, hx_sem, (i % 2, u, k - 1), where)
            copy.start()
            x_sends.append(copy)
        copy = remote(ref, ref, hc_sem, (turn(i), u, 0), {"tensor": peer_t})
        copy.start()
        return x_sends, [copy]

    def fourth(i, u, x_sends, core_sends):
        for k in range(1, nx):
            x_sends[k - 1].wait()
            ref = hid_part(i, u, lax.rem(x + nx - k, nx))
            copy = remote(ref, ref, hc_sem, (turn(i), u, k), {"tensor": peer_t})
            copy.start()
            core_sends.append(copy)
        return core_sends

    def fifth(i, u):
        span = (0, 1) if i == 1 else (i,)
        for j in span:
            for copy in state[j, u]:
                copy.wait()
        if u == local_count:
            if i == 1:
                sdown_load.wait()
            return
        if i == 1:
            down_loads[u].wait()
        lhs = hid[u, pl.ds(i - 1, 2)].reshape(2 * cap, piece)
        result = mm(lhs, down_w[u])
        for j in span:
            n = j - i + 1
            made[step_block(j), pl.ds(u * cap, cap), :] = result[n * cap : (n + 1) * cap].astype(BF16)

    parts = width // cw

    def contribution(b, span):
        return mm(comb[b], made[b, :, span], 0, 0) + mm(s_hid[b], sdown_w[:, span])

    half_rows = tok // 2

    def spans(end):
        return [pl.ds(0, half_rows), pl.ds(half_rows, half_rows)] if end else [pl.ds(0, tok)]

    def rs_copy(upward, b, k, h, end, where):
        d = mir if upward else 1 - mir
        block = phys(b)
        slot = block + 1 - d
        span = (spans(end)[h], pl.ds(k * cw, cw))
        sems, index = (rs_half_sem, (d, k)) if h else (rs_sem, (slot, k))
        return remote(x_all.at[(block,) + span], rs_in.at[(slot,) + span], sems, index, {"expert": where})

    def arrived(upward, b, k, h, end):
        rs_copy(upward, b, k, h, end, above).wait_recv()
        d = mir if upward else 1 - mir
        return rs_in[phys(b) + 1 - d, spans(end)[h], pl.ds(k * cw, cw)].astype(F32)

    early = min(3, parts)

    def originate(r, span):
        @pl.when(zeta == 0)
        def _():
            end = r + 1 == ns
            wide = pl.ds(span[0] * cw, len(span) * cw)
            if not end:
                x_all[phys(r), :, wide] = contribution(phys(r), wide).astype(BF16)
            for k in span:
                if end:
                    one = pl.ds(k * cw, cw)
                    x_all[phys(r), :, one] = contribution(phys(r), one).astype(BF16)
                for h in range(len(spans(end))):
                    rs_copy(True, r, k, h, end, above).start()

    def relay(upward, b, k):
        value = contribution(phys(b), pl.ds(k * cw, cw))
        end = b + 1 == ns if upward else b == 0
        for h, side in enumerate(spans(end)):
            total = value[side.start : side.start + side.size] + arrived(upward, b, k, h, end)
            x_all[phys(b), side, pl.ds(k * cw, cw)] = total.astype(BF16)
            rs_copy(upward, b, k, h, end, above if upward else below).start()

    state = {}

    def run(name, i, u):
        if name == "A":
            state[i, u] = first(i, u)
        elif name == "B":
            state[i, u] = second(i, u, state[i, u])
        elif name == "C":
            state[i, u] = third(i, u, state[i, u])
        elif name == "D":
            state[i, u] = fourth(i, u, *state[i, u])
        else:
            fifth(i, u)

    def inner(i, k):
        if i < ns:
            pl.when(zeta > 0)(functools.partial(arrive, i, k))

    def outer(i, k):
        pl.when(zeta == 0)(functools.partial(arrive, i, k))

    last = units - 1
    late = []
    for i in range(ns):
        if i == 1:
            outer(1, 0)
            arrive(1, 1)
            for copy in meta_copies:
                copy.wait()
        elif i > 1:
            outer(i, 0)
            outer(i, 1)
        dispatch(step_block(i))
        relays = list(range(units)) if i else []
        for u in range(units):
            run("A", i, u)
            if u > 0:
                run("B", i, u - 1)
            if i == 0 and u == 2:
                inner(1, 0)
            if i > 0 and u == 0:
                inner(i + 1, 1)
            if u < 2 and late:
                for v in range(-(-len(late) // (2 - u))):
                    run("C", i - 1, late.pop(0))
            if relays and (i > 2 or u >= 3):
                share = units - 2 if i > 2 and u == 0 else 1 if i > 2 else -(-len(relays) // (units - u))
                for v in range(min(share, len(relays))):
                    run("D", i - 1, relays.pop(0))
        for v in relays:
            run("D", i - 1, v)
        run("C", i, 0)
        rest = list(range(1, units))
        if i > 0:
            inner(i + 2, 0)
        else:
            load_next(len(queue))
        if i < 2:
            run("B", i, last)
            late = rest
            continue
        final = i + 1 == ns
        relays = list(range(units))
        for u in range(units):
            run("E", i - 1, u)
            if u == 0:
                run("B", i, last)
            if u < 2 or u == last - 1:
                run("C", i, rest.pop(0))
        if final:
            run("D", i, relays.pop(0))
            run("D", i, relays.pop(0))
        originate(i - 1, range(early if final else parts))
        for u in rest:
            run("C", i, u)
    done = 0
    for u in relays:
        run("D", ns - 1, u)
        while done < u:
            run("E", ns - 1, done)
            done += 1
            if done == u - 1 and u > 2:
                break
    for u in range(done, units):
        run("E", ns - 1, u)
    originate(ns - 1, range(parts))
    if ns > 2:
        originate(ns - 2, range(early, parts))

    @pl.when(zeta > 0)
    def _():
        for k in range(pieces):
            ag_copy(True, zeta, k, above).wait_send()
            ag_copy(False, zeta, k, below).wait_send()
            for b in range(ns):
                @pl.when(b < zeta)
                def _():
                    ag_copy(True, b, k, above).wait_send()

                @pl.when(b > zeta)
                def _():
                    ag_copy(False, b, k, below).wait_send()

    order = [(r, k) for r in range(2, ns - 2) for k in range(parts)]
    if ns > 3:
        order += [(ns - 2, k) for k in range(early)]
    order += [(ns - 1, k) for k in range(parts)]
    if ns > 3:
        order += [(ns - 2, k) for k in range(early, parts)]
    for n in range(len(order) + 2):
        if n < len(order):
            r, k = order[n]
            pl.when((zeta > 0) & (zeta < r))(functools.partial(relay, True, r, k))
        if n >= 2:
            r, k = order[n - 2]
            if r > ns // 2:
                pl.when(zeta > ns - 1 - r)(functools.partial(relay, False, ns - 1 - r, k))

    def finish(inside):
        for k in range(parts):
            span = pl.ds(k * cw, cw)
            value = contribution(z, span)
            for h, side in enumerate(spans(not inside)):
                total = value[side.start : side.start + side.size] + arrived(False, zeta, k, h, not inside)
                if inside:
                    total = total + arrived(True, zeta, k, h, False)
                out_v[side, span] = total.astype(BF16)
            pltpu.make_async_copy(out_v.at[:, span], out.at[:, span], out_sem).start()

    pl.when(zeta == 0)(functools.partial(finish, False))
    pl.when(zeta > 0)(functools.partial(finish, True))

    @pl.when(zeta == 0)
    def _():
        for k in range(pieces):
            ag_copy(True, zeta, k, above).wait_send()

    def sent(upward, b):
        end = b + 1 == ns if upward else b == 0
        for k in range(parts):
            for h in range(len(spans(end))):
                rs_copy(upward, b, k, h, end, above).wait_send()

    for b in range(ns):
        pl.when(zeta < b)(functools.partial(sent, True, b))
        pl.when(zeta > b)(functools.partial(sent, False, b))
    pltpu.make_async_copy(out_v, out, out_sem).wait()


def local(tokens, choices, affinity, expert_gate, expert_up, expert_down, shared_in, shared_down):
    tok, width = tokens.shape
    top = choices.shape[1]
    ns, nt = lax.axis_size("expert"), lax.axis_size("tensor")
    nx = nt // 2
    piece = min(FFE, expert_gate.shape[1])
    local_count = expert_gate.shape[1] // piece
    hs = shared_in.shape[1]
    hops = ns // 2
    slots = min(3, local_count)
    sigmoids = jax.nn.sigmoid(affinity)
    mix = 2.5 * sigmoids / jnp.sum(sigmoids, axis=1, keepdims=True)
    meta = jnp.concatenate([choices.astype(F32).T, mix.T], axis=0)
    rows = ns * CAP
    srows = ns * tok
    units = local_count + 1
    dims = (ns, nx, local_count, piece, tok, CAP, top)
    hbm = pl.BlockSpec(memory_space=pl.ANY)
    sem = pltpu.SemaphoreType.DMA
    scratch = [
        pltpu.VMEM((ns, tok, width), BF16),
        pltpu.VMEM((ns,) + meta.shape, F32),
        pltpu.VMEM((slots, width, piece), BF16),
        pltpu.VMEM((slots, width, piece), BF16),
        pltpu.VMEM((local_count, piece, width), BF16),
        pltpu.VMEM(shared_in.shape, BF16),
        pltpu.VMEM(shared_down.shape, BF16),
        pltpu.VMEM((local_count, ns, CAP, width), BF16),
        pltpu.VMEM((ns, local_count * CAP, tok), BF16),
        pltpu.VMEM((local_count, 2, rows, piece), BF16),
        pltpu.VMEM((local_count, 2, rows // 2, piece), BF16),
        pltpu.VMEM((local_count, nx - 1, 2, rows // nt, piece), BF16),
        pltpu.VMEM((local_count, nx - 1, 2, rows // nt, piece), BF16),
        pltpu.VMEM((local_count, rows, piece), BF16),
        pltpu.VMEM((2, srows, hs), BF16),
        pltpu.VMEM((2, srows // 2, hs), BF16),
        pltpu.VMEM((nx - 1, 2, srows // nt, hs), BF16),
        pltpu.VMEM((nx - 1, 2, srows // nt, hs), BF16),
        pltpu.VMEM((srows, hs), BF16),
        pltpu.VMEM((2, hops, tok, width), BF16),
        pltpu.VMEM((2, hops, tok, width), BF16),
        sem((4,)),
        sem((local_count,)),
        sem((local_count,)),
        sem((local_count,)),
        sem((2, ns - 1)),
        sem((2, 2, hops)),
        sem((2, units)),
        sem((2, units, nx - 1)),
        sem((2, units, nx - 1)),
        sem((2, units, nx)),
        sem((2, 2, hops)),
    ]
    return pl.pallas_call(
        functools.partial(layer, dims),
        out_shape=jax.ShapeDtypeStruct((tok, width), BF16),
        in_specs=[hbm] * 7,
        out_specs=pl.BlockSpec(memory_space=pltpu.VMEM),
        scratch_shapes=scratch,
        compiler_params=pltpu.CompilerParams(
            collective_id=0, has_side_effects=True, vmem_limit_bytes=60 * 1024 * 1024
        ),
        name="moe_layer",
    )(tokens, meta, expert_gate, expert_up, expert_down, shared_in, shared_down)


def line_local(tokens, choices, affinity, expert_gate, expert_up, expert_down, shared_in, shared_down):
    tok, width = tokens.shape
    top = choices.shape[1]
    ns, nt = lax.axis_size("expert"), lax.axis_size("tensor")
    nx = nt // 2
    piece = min(FFE, expert_gate.shape[1])
    local_count = expert_gate.shape[1] // piece
    hs = shared_in.shape[1]
    pieces = 2
    cw = 256 if width % 256 == 0 else 128
    units = local_count + 1
    dims = (ns, nx, local_count, piece, tok, CAP, top, pieces, cw)
    hbm = pl.BlockSpec(memory_space=pl.ANY)
    sem = pltpu.SemaphoreType.DMA
    scratch = [
        pltpu.VMEM((ns, tok, width), BF16),
        pltpu.VMEM((top, tok), jnp.int32),
        pltpu.VMEM((top, tok), F32),
        pltpu.VMEM((tok, width), BF16),
        pltpu.VMEM((ns, 2 * top, tok), F32),
        pltpu.VMEM((local_count, width, piece), BF16),
        pltpu.VMEM((local_count, width, piece), BF16),
        pltpu.VMEM((local_count, piece, width), BF16),
        pltpu.VMEM(shared_in.shape, BF16),
        pltpu.VMEM(shared_down.shape, BF16),
        pltpu.VMEM((local_count, CAP, width), BF16),
        pltpu.VMEM((ns, local_count * CAP, width), BF16),
        pltpu.VMEM((ns, local_count * CAP, tok), BF16),
        pltpu.VMEM((2, local_count, 2, CAP, piece), BF16),
        pltpu.VMEM((ns, local_count, 2, CAP, piece // 2), BF16),
        pltpu.VMEM((ns, local_count, nx - 1, 2, CAP, piece // nt), BF16),
        pltpu.VMEM((ns, local_count, nx - 1, 2, CAP, piece // nt), BF16),
        pltpu.VMEM((local_count, ns, CAP, piece), BF16),
        pltpu.VMEM((2, 2, tok, hs), BF16),
        pltpu.VMEM((ns, 2, tok // 2, hs), BF16),
        pltpu.VMEM((ns, nx - 1, 2, tok // nt, hs), BF16),
        pltpu.VMEM((ns, nx - 1, 2, tok // nt, hs), BF16),
        pltpu.VMEM((ns, tok, hs), BF16),
        pltpu.VMEM((ns + 1, tok, width), BF16),
        sem((5,)),
        sem((local_count,)),
        sem((local_count,)),
        sem((local_count,)),
        sem((2, ns - 1)),
        sem((2, ns + 1, pieces)),
        sem((2, 2, units)),
        sem((2, 2, units, nx - 1)),
        sem((2, 2, units, nx - 1)),
        sem((2, 3, units, nx)),
        sem((2, ns + 1, width // cw)),
        sem((2, 2, width // cw)),
        sem(()),
    ]
    return pl.pallas_call(
        functools.partial(line_layer, dims),
        out_shape=jax.ShapeDtypeStruct((tok, width), BF16),
        in_specs=[hbm] * 8,
        out_specs=hbm,
        scratch_shapes=scratch,
        compiler_params=pltpu.CompilerParams(
            collective_id=0, has_side_effects=True, vmem_limit_bytes=65400 * 1024
        ),
        name="moe_line",
    )(tokens, choices.T, affinity.T, expert_gate, expert_up, expert_down, shared_in, shared_down)


def choose(tokens, choices, affinity, expert_gate, *rest):
    tok = tokens.shape[0]
    ns, nt = lax.axis_size("expert"), lax.axis_size("tensor")
    piece = min(FFE, expert_gate.shape[1])
    fits = ns % 2 == 0 and ns > 2 and piece % (128 * nt) == 0 and tok % (16 * nt) == 0 and expert_gate.shape[1] % piece == 0
    which = line_local if fits else local
    return which(tokens, choices, affinity, expert_gate, *rest)


def solution(mesh):
    placed = (
        P(("groups", "expert"), "tensor"),
        P(("groups", "expert"), None),
        P(("groups", "expert"), None),
        P("tensor", "expert"),
        P("tensor", "expert"),
        P("expert", "tensor"),
        P(None, "expert", "tensor"),
        P("expert", "tensor"),
    )
    return jax.shard_map(
        choose,
        mesh=mesh,
        in_specs=placed,
        out_specs=P(("groups", "expert"), "tensor"),
        check_vma=False,
    )
```
